32 devices in a mesh: gx: 4 (over y, core), gy: 2 (over x), gz: 4 (over z).
Axes of the slice: x: 2, y: 2, z: 4, core: 2. Of those that a mesh axis runs over, the one named last changes fastest.
Arguments:
- euler_state: float32 [5, 16, 16, 512], P(None, 'gx', 'gy', 'gz'), as said below
- gravity_state: float32 [4, 16, 16, 512], P(None, 'gx', 'gy', 'gz'), may hold values from -6 to 6
Outputs:
- section_rate: float32 [5, 16, 16, 512], P(None, 'gx', 'gy', 'gz')
- gravity_next: float32 [4, 16, 16, 512], P(None, 'gx', 'gy', 'gz')
- gravity_source: float32 [4, 16, 16, 512], P(None, 'gx', 'gy', 'gz')
- residual_norm: float32 [], replicated
The draws below stay inside these ranges and needn't reach their ends.
Inputs may be any that keep to these rules, and one draw needn't show every extreme that they name: `euler_state`: each node's density lies between 0.7 and 3.9 and its pressure, for a ratio of specific heats of 1.4, between 0.7 and 71.
All inputs are finite; a program needn't handle non-finite values.
Results may differ from the reference program's by a relative error of at most 0.0003.
Values sent between devices are 32-bit elements; how exact they have to be, the bound alone decides.
A program may use at most 64 MiB of HBM per device.

```python
import math
import jax
import jax.numpy as jnp
import numpy as np
from jax import lax

GRAV_VARS = 4
ITERS = 3
NXN = 16
NYN = 16
NZN = 512


def draw_euler_state(key, part):
    subkeys = jax.random.split(jax.random.fold_in(key, 17), 5)
    grid_shape = (NXN, NYN, NZN)
    block_shape = (NXN // 4, NYN // 4, NZN // 4)
    log_rough = jax.random.uniform(subkeys[0], block_shape, jnp.float32, math.log(0.001), math.log(0.3))
    roughness = jnp.exp(log_rough)
    roughness = jnp.repeat(jnp.repeat(jnp.repeat(roughness, 4, axis=0), 4, axis=1), 4, axis=2)
    height = lax.broadcasted_iota(jnp.int32, grid_shape, 2).astype(jnp.float32) / NZN
    across = lax.broadcasted_iota(jnp.int32, grid_shape, 0).astype(jnp.float32) / NXN
    wiggle_rho = jax.random.uniform(subkeys[1], grid_shape, jnp.float32, -1.0, 1.0)
    wiggle_pres = jax.random.uniform(subkeys[2], grid_shape, jnp.float32, -1.0, 1.0)
    base_rho = 1.0 + height + across
    velocity = 0.3 * jax.random.uniform(subkeys[3], (3,) + grid_shape, jnp.float32, -1.0, 1.0)
    hot_block = jax.random.randint(subkeys[4], (3,), 0, jnp.array(block_shape, dtype=jnp.int32))
    block_x = lax.broadcasted_iota(jnp.int32, grid_shape, 0) // 4
    block_y = lax.broadcasted_iota(jnp.int32, grid_shape, 1) // 4
    block_z = lax.broadcasted_iota(jnp.int32, grid_shape, 2) // 4
    is_hot = (block_x == hot_block[0]) & (block_y == hot_block[1]) & (block_z == hot_block[2])
    density = base_rho * (1.0 + roughness * wiggle_rho)
    pressure = (1.0 + 8.0 * height) * (1.0 + roughness * wiggle_pres) * jnp.where(is_hot, 6.0, 1.0)
    energy = pressure / 0.4 + 0.5 * density * jnp.sum(velocity * velocity, axis=0)
    return jnp.concatenate([density[None], density[None] * velocity, energy[None]], axis=0)


def levels(own_key, extent, shards, smallest, top_value):
    loudness, own = 1.0, jax.random.fold_in(own_key, 6)
    for axis_at, blocks in shards:
        draws = jnp.exp(jax.random.uniform(jax.random.fold_in(own, axis_at), (blocks,), jnp.float32, smallest / len(shards), top_value / len(shards)))
        loudness = loudness * jnp.repeat(draws, extent[axis_at] // blocks).reshape([-1 if axis == axis_at else 1 for axis in range(len(extent))])
    return loudness


def gaussian(stream_key, extent, width, most, shards=(), held_as=jnp.bfloat16):
    level = levels(stream_key, extent, shards, -0.22, 0.18) if shards else 1.0
    result = jax.random.normal(stream_key, extent, jnp.float32) * width * level
    return jnp.minimum(jnp.maximum(result, -most), most).astype(held_as)


def setup_inputs(seed: int = 0) -> dict:
    splits = jax.random.split(jax.random.key(seed), 3)
    return {
        "euler_state": draw_euler_state(jax.random.fold_in(splits[2], 71), 0),
        "gravity_state": gaussian(splits[1], (GRAV_VARS, NXN, NYN, NZN), 1.0, 6.0, ((1, 4), (2, 2), (3, 4)), jnp.float32),
    }


gamma_gas = 1.4
elem_width = 1.0
cfl_euler = 0.5
alpha_most = 0.5
indicator_level = 0.5 * 10.0 ** (-1.8 * 4.0 ** 0.25)
indicator_slope = math.log((1.0 - 0.0001) / 0.0001) / indicator_level
coupling = 10.0
relax_time = 1.0
grav_speed = 1.0
pseudo_step = 0.3 * elem_width / 7.0

def lgl_tables():
    points = np.array([-1.0, -1.0 / math.sqrt(5.0), 1.0 / math.sqrt(5.0), 1.0])
    weights = np.array([1.0, 5.0, 5.0, 1.0]) / 6.0
    barycentric = np.array([1.0 / np.prod([points[node_a] - points[node_b] for node_b in range(4) if node_b != node_a]) for node_a in range(4)])
    derivative = np.zeros((4, 4))
    for node_a in range(4):
        for node_b in range(4):
            if node_b != node_a:
                derivative[node_a, node_b] = barycentric[node_b] / barycentric[node_a] / (points[node_a] - points[node_b])
        derivative[node_a, node_a] = -np.sum(derivative[node_a])
    legendre = np.stack([np.ones(4), points, 0.5 * (3.0 * points ** 2 - 1.0), 0.5 * (5.0 * points ** 3 - 3.0 * points)], axis=1)
    legendre = legendre * np.sqrt((2.0 * np.arange(4) + 1.0) / 2.0)
    gram = np.sum(weights[:, None] * legendre * legendre, axis=0)
    modal_map = (legendre * weights[:, None]).T / gram[:, None]
    return (weights, derivative, modal_map)

def diagonal_of(derivative):
    return [derivative[node_at, node_at] for node_at in range(4)]

def along(values, length, axis_pos, array_rank):
    shape_list = [1] * array_rank
    shape_list[axis_pos] = length
    return jnp.asarray(np.tile(np.asarray([float(item) for item in values]), length // 4).reshape(shape_list))

def log_mean(left, right):
    ratio_sq = ((left - right) / (left + right)) ** 2
    is_close = ratio_sq < 0.0001
    series = (left + right) / (2.0 + ratio_sq * (2.0 / 3.0 + ratio_sq * (2.0 / 5.0 + ratio_sq * 2.0 / 7.0)))
    top_part = jnp.where(is_close, 1.0, right - left)
    low_part = jnp.where(is_close, 1.0, jnp.log(right / left))
    return jnp.where(is_close, series, top_part / low_part)

def describe(conserved, direction):
    density = conserved[0]
    velocity = conserved[1:4] / density
    pressure = (gamma_gas - 1.0) * (conserved[4] - 0.5 * lax.optimization_barrier(jnp.sum(conserved[1:4] * velocity, axis=0)))
    normal_vel = velocity[direction]
    momentum_flux = [conserved[1 + comp] * normal_vel + (pressure if comp == direction else 0.0) for comp in range(3)]
    energy_flux = (conserved[4] + pressure) * normal_vel
    sound = jnp.sqrt(gamma_gas * pressure / density)
    return jnp.stack([conserved[0], conserved[1], conserved[2], conserved[3], conserved[4], velocity[0], velocity[1], velocity[2], pressure, conserved[1 + direction]] + momentum_flux + [energy_flux, jnp.abs(normal_vel) + sound])

def euler_interface(left, right):
    speed = jnp.maximum(left[14], right[14])
    return 0.5 * (left[9:14] + right[9:14]) - 0.5 * speed * (right[0:5] - left[0:5])

def two_point(left, right, direction):
    rho_mean = log_mean(left[0], right[0])
    inv_mean = left[8] * right[8] / log_mean(left[0] * right[8], right[0] * left[8])
    vel_avg = 0.5 * (left[5:8] + right[5:8])
    pres_avg = 0.5 * (left[8] + right[8])
    vel_product = 0.5 * lax.optimization_barrier(jnp.sum(left[5:8] * right[5:8], axis=0))
    mass_flux = rho_mean * vel_avg[direction]
    momentum = [mass_flux * vel_avg[comp] + (pres_avg if comp == direction else 0.0) for comp in range(3)]
    energy = mass_flux * (vel_product + inv_mean / (gamma_gas - 1.0)) + 0.5 * (left[8] * right[5 + direction] + right[8] * left[5 + direction])
    return jnp.stack([mass_flux] + momentum + [energy])

def euler_direction(described, low_desc, high_desc, direction):
    weights, derivative, modal_map = lgl_tables()
    axis_pos = direction + 1
    length = described.shape[axis_pos]
    array_rank = described.ndim
    prev_desc = jnp.concatenate([low_desc, lax.slice_in_dim(described, 0, length - 1, axis=axis_pos)], axis=axis_pos)
    face_flux = euler_interface(prev_desc, described)
    last_face = euler_interface(lax.slice_in_dim(described, length - 1, length, axis=axis_pos), high_desc)
    next_faces = jnp.concatenate([lax.slice_in_dim(face_flux, 1, length, axis=axis_pos), last_face], axis=axis_pos)
    own_flux = described[9:14]
    volume = along([2.0 * item for item in diagonal_of(derivative)], length, axis_pos, array_rank) * own_flux
    for offset in range(1, 4):
        partner = jnp.roll(described, -offset, axis=axis_pos)
        pair_flux = two_point(described, partner, direction)
        upward = [2.0 * derivative[node_at, node_at + offset] if node_at + offset < 4 else 0.0 for node_at in range(4)]
        downward = [2.0 * derivative[node_at, node_at - offset] if node_at - offset >= 0 else 0.0 for node_at in range(4)]
        volume = volume + along(upward, length, axis_pos, array_rank) * pair_flux + along(downward, length, axis_pos, array_rank) * jnp.roll(pair_flux, offset, axis=axis_pos)
    first_coef = along([-1.0 / weights[0], 0.0, 0.0, 0.0], length, axis_pos, array_rank)
    last_coef = along([0.0, 0.0, 0.0, 1.0 / weights[3]], length, axis_pos, array_rank)
    dg_part = volume + first_coef * (face_flux - own_flux) + last_coef * (next_faces - own_flux)
    fv_part = along(1.0 / weights, length, axis_pos, array_rank) * (next_faces - face_flux)
    return (dg_part, fv_part)

def section_rate_from(euler_state, gravity_state, low_states, high_states, alpha):
    dg_total = 0.0
    fv_total = 0.0
    speed_total = 0.0
    for direction in range(3):
        described = describe(euler_state, direction)
        dg_part, fv_part = euler_direction(described, describe(low_states[direction], direction), describe(high_states[direction], direction), direction)
        dg_total = dg_total + dg_part
        fv_total = fv_total + fv_part
        speed_total = speed_total + described[14]
    grav_grad = gravity_state[1:4]
    source = jnp.concatenate([jnp.zeros_like(euler_state[0:1]), -euler_state[0:1] * grav_grad, -lax.optimization_barrier(jnp.sum(euler_state[1:4] * grav_grad, axis=0, keepdims=True))], axis=0)
    rate = -(2.0 / elem_width) * ((1.0 - alpha) * dg_total + alpha * fv_total) + source
    return (rate, speed_total)

def gravity_flux(gravity, direction):
    zero_field = jnp.zeros_like(gravity[0])
    parts = [-gravity[1 + direction]]
    for comp in range(3):
        parts.append(-gravity[0] / relax_time if comp == direction else zero_field)
    return jnp.stack(parts)

def gravity_interface(left, right, direction):
    return 0.5 * (gravity_flux(left, direction) + gravity_flux(right, direction)) - 0.5 * grav_speed * (right - left)

def gravity_direction(gravity, first_face, end_face, direction):
    weights, derivative, modal_map = lgl_tables()
    axis_pos = direction + 1
    length = gravity.shape[axis_pos]
    array_rank = gravity.ndim
    own_flux = gravity_flux(gravity, direction)
    inner = gravity_interface(jnp.roll(gravity, 1, axis=axis_pos), gravity, direction)
    face_flux = jnp.concatenate([first_face, lax.slice_in_dim(inner, 1, length, axis=axis_pos)], axis=axis_pos)
    next_faces = jnp.concatenate([lax.slice_in_dim(face_flux, 1, length, axis=axis_pos), end_face], axis=axis_pos)
    volume = along(diagonal_of(derivative), length, axis_pos, array_rank) * own_flux
    for offset in range(1, 4):
        upward = [derivative[node_at, node_at + offset] if node_at + offset < 4 else 0.0 for node_at in range(4)]
        downward = [derivative[node_at, node_at - offset] if node_at - offset >= 0 else 0.0 for node_at in range(4)]
        volume = volume + along(upward, length, axis_pos, array_rank) * jnp.roll(own_flux, -offset, axis=axis_pos) + along(downward, length, axis_pos, array_rank) * jnp.roll(own_flux, offset, axis=axis_pos)
    first_coef = along([-1.0 / weights[0], 0.0, 0.0, 0.0], length, axis_pos, array_rank)
    last_coef = along([0.0, 0.0, 0.0, 1.0 / weights[3]], length, axis_pos, array_rank)
    return volume + first_coef * (face_flux - own_flux) + last_coef * (next_faces - own_flux)

def gravity_rate(gravity, first_faces, end_faces, density, density_mean):
    total = 0.0
    for direction in range(3):
        total = total + gravity_direction(gravity, first_faces[direction], end_faces[direction], direction)
    rate = -(2.0 / elem_width) * total
    rate_phi = rate[0:1] - coupling * (density[None] - density_mean)
    rate_grad = rate[1:4] - gravity[1:4] / relax_time
    return jnp.concatenate([rate_phi, rate_grad], axis=0)

def node_weights(grid_shape):
    weights, derivative, modal_map = lgl_tables()
    return along(weights, grid_shape[0], 0, 3) * along(weights, grid_shape[1], 1, 3) * along(weights, grid_shape[2], 2, 3)

def element_alpha(euler_state):
    weights, derivative, modal_map = lgl_tables()
    density = euler_state[0]
    velocity = euler_state[1:4] / density
    pressure = (gamma_gas - 1.0) * (euler_state[4] - 0.5 * lax.optimization_barrier(jnp.sum(euler_state[1:4] * velocity, axis=0)))
    product = density * pressure
    size_x, size_y, size_z = product.shape
    blocks = product.reshape(size_x // 4, 4, size_y // 4, 4, size_z // 4, 4)
    modal_arr = jnp.asarray(modal_map)
    coeffs = jnp.einsum('ai,bj,ck,xiyjzk->xaybzc', modal_arr, modal_arr, modal_arr, blocks, precision=lax.Precision.HIGHEST)
    energy = coeffs * coeffs
    low_index = np.array([1.0, 1.0, 1.0, 0.0])
    low_mask = jnp.asarray(low_index.reshape(1, 4, 1, 1, 1, 1) * low_index.reshape(1, 1, 1, 4, 1, 1) * low_index.reshape(1, 1, 1, 1, 1, 4))
    total = lax.optimization_barrier(jnp.sum(energy, axis=(1, 3, 5)))
    high_energy = lax.optimization_barrier(jnp.sum(energy * (1.0 - low_mask), axis=(1, 3, 5)))
    high_share = high_energy / total
    alpha = alpha_most / (1.0 + jnp.exp(-indicator_slope * (high_share - indicator_level)))
    return jnp.repeat(jnp.repeat(jnp.repeat(alpha, 4, axis=0), 4, axis=1), 4, axis=2)

def reference(euler_state, gravity_state):
    low_states = []
    high_states = []
    for direction in range(3):
        length = euler_state.shape[direction + 1]
        low_states.append(lax.slice_in_dim(euler_state, length - 1, length, axis=direction + 1))
        high_states.append(lax.slice_in_dim(euler_state, 0, 1, axis=direction + 1))
    alpha = element_alpha(euler_state)
    rate, speed_total = section_rate_from(euler_state, gravity_state, low_states, high_states, alpha)
    time_step = cfl_euler * elem_width / (7.0 * jnp.max(speed_total))
    state_next = euler_state + time_step * rate
    grid_shape = euler_state.shape[1:]
    weight_grid = node_weights(grid_shape)
    weight_total = 8.0 * (grid_shape[0] // 4) * (grid_shape[1] // 4) * (grid_shape[2] // 4)
    density_mean = jnp.sum(weight_grid * state_next[0]) / weight_total
    gravity = gravity_state
    rate_grav = jnp.zeros_like(gravity_state)
    for iteration in range(ITERS):
        first_faces = []
        end_faces = []
        for direction in range(3):
            length = gravity.shape[direction + 1]
            first_plane = lax.slice_in_dim(gravity, 0, 1, axis=direction + 1)
            last_plane = lax.slice_in_dim(gravity, length - 1, length, axis=direction + 1)
            first_faces.append(gravity_interface(last_plane, first_plane, direction))
            end_faces.append(gravity_interface(last_plane, first_plane, direction))
        rate_grav = gravity_rate(gravity, first_faces, end_faces, state_next[0], density_mean)
        gravity = gravity + pseudo_step * rate_grav
    residual_norm = jnp.sqrt(jnp.sum(weight_grid * rate_grav[0] * rate_grav[0]) / weight_total)
    grav_grad = gravity[1:4]
    gravity_source = jnp.concatenate([-state_next[0:1] * grav_grad, -lax.optimization_barrier(jnp.sum(state_next[1:4] * grav_grad, axis=0, keepdims=True))], axis=0)
    return (rate, gravity, gravity_source, residual_norm)
```

```python
import itertools
import math

import jax
import jax.numpy as jnp
import numpy as np
from jax import lax
from jax.experimental import pallas as pl
from jax.experimental.pallas import tpu as pltpu
from jax.sharding import PartitionSpec as P

ITERS = 3
AXES = ("gx", "gy", "gz")
MOST_PARTNERS = 64

gamma_gas = 1.4
elem_width = 1.0
cfl_euler = 0.5
alpha_most = 0.5
indicator_level = 0.5 * 10.0 ** (-1.8 * 4.0**0.25)
indicator_slope = math.log((1.0 - 0.0001) / 0.0001) / indicator_level
coupling = 10.0
relax_time = 1.0
grav_speed = 1.0
pseudo_step = 0.3 * elem_width / 7.0
MESH = pl.DeviceIdType.MESH


def lgl_tables():
    points = np.array([-1.0, -1.0 / math.sqrt(5.0), 1.0 / math.sqrt(5.0), 1.0])
    weights = np.array([1.0, 5.0, 5.0, 1.0]) / 6.0
    barycentric = np.array(
        [
            1.0
            / np.prod([points[node_a] - points[node_b] for node_b in range(4) if node_b != node_a])
            for node_a in range(4)
        ]
    )
    derivative = np.zeros((4, 4))
    for node_a in range(4):
        for node_b in range(4):
            if node_b != node_a:
                derivative[node_a, node_b] = (
                    barycentric[node_b] / barycentric[node_a] / (points[node_a] - points[node_b])
                )
        derivative[node_a, node_a] = -np.sum(derivative[node_a])
    legendre = np.stack(
        [np.ones(4), points, 0.5 * (3.0 * points**2 - 1.0), 0.5 * (5.0 * points**3 - 3.0 * points)],
        axis=1,
    )
    legendre = legendre * np.sqrt((2.0 * np.arange(4) + 1.0) / 2.0)
    gram = np.sum(weights[:, None] * legendre * legendre, axis=0)
    modal_map = (legendre * weights[:, None]).T / gram[:, None]
    return (weights, derivative, modal_map)


WEIGHTS, DERIV, MODAL = lgl_tables()
DERIV_FOLDED = DERIV.copy()
DERIV_FOLDED[0, 0] += 1.0 / WEIGHTS[0]
DERIV_FOLDED[3, 3] -= 1.0 / WEIGHTS[3]
SELF_COEF = 2.0 * np.diag(DERIV)
SELF_COEF[0] += 1.0 / WEIGHTS[0]
SELF_COEF[3] -= 1.0 / WEIGHTS[3]


def reduce_stages(sizes):
    total = math.prod(sizes[axis] for axis in AXES)
    if total <= MOST_PARTNERS:
        return [AXES]
    return [("gx", "gy"), ("gz",)]


def offsets_of(axes, sizes):
    ranges = [range(sizes[axis]) for axis in axes]
    return [item for item in itertools.product(*ranges) if any(item)]


class Plane:
    def __init__(self, ny, nz):
        self.shape = (ny, nz)
        self.index = [lax.broadcasted_iota(jnp.int32, (ny, nz), axis) for axis in range(2)]
        self.node = [item & 3 for item in self.index]
        self.is_node = [[node == value for value in range(4)] for node in self.node]
        self.cache = {}

    def coef(self, values, axis):
        values = tuple(float(np.float32(value)) for value in values)
        if len(set(values)) == 1:
            return values[0]
        key = (values, axis)
        if key not in self.cache:
            result = jnp.full(self.shape, values[3], jnp.float32)
            for node in range(2, -1, -1):
                result = jnp.where(self.is_node[axis][node], values[node], result)
            self.cache[key] = result
        return self.cache[key]

    def ahead(self, value, by, axis):
        return pltpu.roll(value, (-by) % self.shape[axis], axis)

    def apply(self, matrix, value, axis):
        total = self.coef(np.diag(matrix), axis) * value
        for by in range(1, 4):
            up = [matrix[node, node + by] if node + by < 4 else 0.0 for node in range(4)]
            down = [matrix[node, node - by] if node - by >= 0 else 0.0 for node in range(4)]
            total = total + self.coef(up, axis) * self.ahead(value, by, axis)
            total = total + self.coef(down, axis) * self.ahead(value, -by, axis)
        return total

    def previous(self, value, halo, axis):
        return jnp.where(self.index[axis] == 0, halo, self.ahead(value, -1, axis))

    def following(self, value, halo, axis):
        last = self.shape[axis] - 1
        return jnp.where(self.index[axis] == last, halo, self.ahead(value, 1, axis))


def primitive(state):
    inverse = 1.0 / state[0]
    vel = [state[1 + comp] * inverse for comp in range(3)]
    kinetic = state[1] * vel[0] + state[2] * vel[1] + state[3] * vel[2]
    pressure = (gamma_gas - 1.0) * (state[4] - 0.5 * kinetic)
    sound = jnp.sqrt(gamma_gas * pressure * inverse)
    return list(state) + vel + [pressure, sound]


def flux_of(node, direction):
    normal = node[5 + direction]
    momentum = [
        node[1 + comp] * normal + node[8] if comp == direction else node[1 + comp] * normal
        for comp in range(3)
    ]
    return [node[1 + direction]] + momentum + [(node[4] + node[8]) * normal]


def euler_interface(left, right, direction):
    speed = 0.5 * jnp.maximum(
        jnp.abs(left[5 + direction]) + left[9], jnp.abs(right[5 + direction]) + right[9]
    )
    flux_left, flux_right = flux_of(left, direction), flux_of(right, direction)
    return [
        0.5 * (flux_left[var] + flux_right[var]) - speed * (right[var] - left[var])
        for var in range(5)
    ]


def log_mean_parts(left, right):
    total = left + right
    ratio = (left - right) / total
    ratio_sq = ratio * ratio
    is_close = ratio_sq < 0.0001
    series = 2.0 + ratio_sq * (2.0 / 3.0 + ratio_sq * (2.0 / 5.0 + ratio_sq * (2.0 / 7.0)))
    top = jnp.where(is_close, total, right - left)
    low = jnp.where(is_close, series, jnp.log(right / left))
    return top, low


def two_point(left, right, direction):
    top, low = log_mean_parts(left[0], right[0])
    rho_mean = top / low
    top, low = log_mean_parts(left[0] * right[4], right[0] * left[4])
    inv_mean = left[4] * right[4] * low / top
    vel_avg = [0.5 * (left[1 + comp] + right[1 + comp]) for comp in range(3)]
    pres_avg = 0.5 * (left[4] + right[4])
    vel_product = 0.5 * (left[1] * right[1] + left[2] * right[2] + left[3] * right[3])
    mass = rho_mean * vel_avg[direction]
    momentum = [
        mass * vel_avg[comp] + pres_avg if comp == direction else mass * vel_avg[comp]
        for comp in range(3)
    ]
    energy = mass * (vel_product + inv_mean * (1.0 / (gamma_gas - 1.0))) + 0.5 * (
        left[4] * right[1 + direction] + right[4] * left[1 + direction]
    )
    return [mass] + momentum + [energy]


def gravity_interface(left, right, direction):
    result = []
    for var in range(4):
        jump = 0.5 * grav_speed * (right[var] - left[var])
        if var == 0:
            result.append(-0.5 * (left[1 + direction] + right[1 + direction]) - jump)
        elif var == 1 + direction:
            result.append(-(0.5 / relax_time) * (left[0] + right[0]) - jump)
        else:
            result.append(-jump)
    return result


def add_volume(volume, nodes, plane, nx):
    pair_fields = [[node[0], node[5], node[6], node[7], node[8]] for node in nodes]

    def add(x, terms):
        for var in range(5):
            old = volume[var][x]
            volume[var][x] = terms[var] if old is None else old + terms[var]

    for start in range(0, nx, 4):
        for low in range(4):
            own = flux_of(nodes[start + low], 0)
            coef = float(np.float32(SELF_COEF[low]))
            add(start + low, [coef * item for item in own])
            for high in range(low + 1, 4):
                flux = two_point(pair_fields[start + low], pair_fields[start + high], 0)
                add(start + low, [float(2.0 * DERIV[low, high]) * item for item in flux])
                add(start + high, [float(2.0 * DERIV[high, low]) * item for item in flux])
    deriv = 2.0 * DERIV
    for axis in range(2):
        direction = axis + 1
        for x in range(nx):
            here = pair_fields[x]
            own = flux_of(nodes[x], direction)
            coef = plane.coef(SELF_COEF, axis)
            add(x, [coef * item for item in own])
            there = [plane.ahead(item, 1, axis) for item in here]
            flux = two_point(here, there, direction)
            up = plane.coef([deriv[0, 1], deriv[1, 2], deriv[2, 3], 0.0], axis)
            down = plane.coef([0.0, deriv[1, 0], deriv[2, 1], deriv[3, 2]], axis)
            add(x, [up * item + down * plane.ahead(item, -1, axis) for item in flux])
            is_last = plane.is_node[axis][3]
            there = [
                jnp.where(is_last, plane.ahead(item, -3, axis), plane.ahead(item, 2, axis))
                for item in here
            ]
            flux = two_point(here, there, direction)
            own_coef = plane.coef([deriv[0, 2], deriv[1, 3], 0.0, deriv[3, 0]], axis)
            down = plane.coef([0.0, 0.0, deriv[2, 0], deriv[3, 1]], axis)
            up = plane.coef([deriv[0, 3], 0.0, 0.0, 0.0], axis)
            add(
                x,
                [
                    own_coef * item
                    + down * plane.ahead(item, -2, axis)
                    + up * plane.ahead(item, 3, axis)
                    for item in flux
                ],
            )


def element_alpha(nodes, plane, nx):
    ones = np.ones((4, 4))
    low_index = np.array([1.0, 1.0, 1.0, 0.0])
    not_low = 1.0 - plane.coef(low_index, 0) * plane.coef(low_index, 1)
    result = []
    for start in range(0, nx, 4):
        product = [nodes[start + node][0] * nodes[start + node][8] for node in range(4)]
        energies = []
        for mode in range(4):
            coeffs = sum(float(MODAL[mode, node]) * product[node] for node in range(4))
            coeffs = plane.apply(MODAL, plane.apply(MODAL, coeffs, 0), 1)
            energies.append(coeffs * coeffs)
        low_part = energies[0] + energies[1] + energies[2]
        sums = [low_part + energies[3], low_part * not_low + energies[3]]
        sums = [plane.apply(ones, plane.apply(ones, item, 1), 0) for item in sums]
        share = sums[1] / sums[0]
        alpha = alpha_most / (1.0 + jnp.exp(-indicator_slope * (share - indicator_level)))
        result += [alpha] * 4
    return result


def make_kernel(sizes, shape):
    nx, ny, nz = shape
    stages = reduce_stages(sizes)
    weight_total = (
        8.0 * (nx // 4) * (ny // 4) * (nz // 4) * math.prod(sizes[axis] for axis in AXES)
    )

    def kernel(
        euler_hbm,
        gravity_hbm,
        rate_ref,
        grav_ref,
        source_ref,
        norm_ref,
        euler_ref,
        grav_bufs,
        halo_xe,
        halo_xg,
        send_y,
        recv_y,
        send_z,
        recv_z,
        reduce_send,
        *rest,
    ):
        reduce_recv = rest[: len(stages)]
        load_sem, send_sem, recv_sem, reduce_send_sem, reduce_recv_sem = rest[len(stages) :]
        place = {axis: lax.axis_index(axis) for axis in AXES}

        def moved(axis, by):
            size = sizes[axis]
            by = by % size
            if by == 0:
                return place[axis]
            target = place[axis] + by
            return jnp.where(target >= size, target - size, target)

        targets = {axis: [moved(axis, by) for by in range(sizes[axis])] for axis in AXES}

        def device(axes, offset):
            return {axis: targets[axis][by] for axis, by in zip(axes, offset)}

        barrier = pltpu.get_barrier_semaphore()
        count = 0
        for axes in stages:
            for offset in offsets_of(axes, sizes):
                pl.semaphore_signal(
                    barrier, inc=1, device_id=device(axes, offset), device_id_type=MESH
                )
                count += 1
        load_euler = pltpu.make_async_copy(euler_hbm, euler_ref, load_sem.at[0])
        load_gravity = pltpu.make_async_copy(gravity_hbm, grav_bufs.at[0], load_sem.at[1])
        load_euler.start()
        load_gravity.start()
        load_euler.wait()
        load_gravity.wait()

        plane = Plane(ny, nz)
        state = [[euler_ref[var, x] for x in range(nx)] for var in range(5)]
        grav = [[grav_bufs[0, var, x] for x in range(nx)] for var in range(4)]

        def pack(round_at, fields):
            lanes = [jnp.zeros((ny, nz), jnp.float32) for side in range(2)]
            for at, item in enumerate(itertools.chain(*fields)):
                send_y[round_at, 0, at : at + 1, :] = item[ny - 1 : ny, :]
                send_y[round_at, 1, at : at + 1, :] = item[0:1, :]
                here = plane.index[1] == at
                lanes[0] = jnp.where(here, plane.ahead(item, nz - 1 - at, 1), lanes[0])
                lanes[1] = jnp.where(here, plane.ahead(item, -at, 1), lanes[1])
            send_z[round_at, 0] = lanes[0]
            send_z[round_at, 1] = lanes[1]

        def exchange(round_at):
            copies = []

            def send(src, dst, slot, axis, by):
                copy = pltpu.make_async_remote_copy(
                    src_ref=src,
                    dst_ref=dst,
                    send_sem=send_sem.at[round_at, slot],
                    recv_sem=recv_sem.at[round_at, slot],
                    device_id=device((axis,), (by % sizes[axis],)),
                    device_id_type=MESH,
                )
                copy.start()
                copies.append(copy)

            for side, by in ((0, 1), (1, -1)):
                face = nx - 1 if side == 0 else 0
                if round_at == 0:
                    send(euler_ref.at[:, face], halo_xe.at[side], 6 + side, "gx", by)
                send(
                    grav_bufs.at[round_at, :, face], halo_xg.at[round_at, side], side, "gx", by
                )
                rows = recv_y.shape[2] if round_at == 0 else 8 * ((4 * nx + 7) // 8)
                send(
                    send_y.at[round_at, side, pl.ds(0, rows)],
                    recv_y.at[round_at, side, pl.ds(0, rows)],
                    2 + side,
                    "gy",
                    by,
                )
                send(send_z.at[round_at, side], recv_z.at[round_at, side], 4 + side, "gz", by)
            return copies

        def halo_y(round_at, side, at):
            return jnp.broadcast_to(recv_y[round_at, side, at : at + 1, :], (ny, nz))

        def halo_z(column, at):
            return jnp.broadcast_to(column[:, at : at + 1], (ny, nz))

        def reduce_start(round_at, stage_at, rows):
            axes = stages[stage_at]
            for at, row in enumerate(rows):
                reduce_send[round_at, stage_at, at] = row
            copies = []
            for slot, offset in enumerate(offsets_of(axes, sizes)):
                copy = pltpu.make_async_remote_copy(
                    src_ref=reduce_send.at[round_at, stage_at, pl.ds(0, len(rows))],
                    dst_ref=reduce_recv[stage_at].at[round_at, slot, pl.ds(0, len(rows))],
                    send_sem=reduce_send_sem.at[round_at, stage_at],
                    recv_sem=reduce_recv_sem.at[round_at, stage_at],
                    device_id=device(axes, offset),
                    device_id_type=MESH,
                )
                copy.start()

        def reduce_finish(round_at, rows, combine):
            for stage_at in range(len(stages)):
                if stage_at > 0:
                    reduce_start(round_at, stage_at, rows)
                got = reduce_recv[stage_at].at[round_at, :, pl.ds(0, len(rows))]
                pltpu.make_async_copy(got, got, reduce_recv_sem.at[round_at, stage_at]).wait()
                pltpu.make_async_copy(got, got, reduce_send_sem.at[round_at, stage_at]).wait()
                partners = reduce_recv[stage_at].shape[1]
                new_rows = []
                for at, row in enumerate(rows):
                    parts = [row] + [
                        reduce_recv[stage_at][round_at, slot, at] for slot in range(partners)
                    ]
                    while len(parts) > 1:
                        pairs = [
                            combine[at](parts[item], parts[item + 1])
                            for item in range(0, len(parts) - 1, 2)
                        ]
                        parts = pairs + ([parts[-1]] if len(parts) % 2 else [])
                    new_rows.append(parts[0])
                rows = new_rows
            return rows

        pack(0, state + grav)
        nodes = [primitive([state[var][x] for var in range(5)]) for x in range(nx)]
        weight_yz = plane.coef(WEIGHTS, 0) * plane.coef(WEIGHTS, 1)

        def weighted_row(items):
            total = sum(float(WEIGHTS[x % 4]) * items[x] for x in range(nx))
            return jnp.sum(weight_yz * total, axis=0, keepdims=True)

        speeds = [
            jnp.abs(node[5]) + jnp.abs(node[6]) + jnp.abs(node[7]) + 3.0 * node[9] for node in nodes
        ]
        fastest = speeds[0]
        for item in speeds[1:]:
            fastest = jnp.maximum(fastest, item)
        first_rows = [jnp.max(fastest, axis=0, keepdims=True), weighted_row(state[0])]

        pl.semaphore_wait(barrier, count)
        copies_0 = exchange(0)
        reduce_start(0, 0, first_rows)

        alpha = element_alpha(nodes, plane, nx)
        volume = [[None] * nx for var in range(5)]
        add_volume(volume, nodes, plane, nx)
        total = [[(1.0 - alpha[x]) * volume[var][x] for x in range(nx)] for var in range(5)]

        for copy in copies_0:
            copy.wait()

        def face_coefs(axis, alpha_x):
            start = jnp.where(plane.is_node[axis][0], 1.0, alpha_x)
            stop = jnp.where(plane.is_node[axis][3], 1.0, alpha_x)
            inverse = plane.coef(1.0 / WEIGHTS, axis)
            return start * inverse, stop * inverse

        edges = [primitive([halo_xe[side, var] for var in range(5)]) for side in range(2)]
        row = [edges[0]] + nodes + [edges[1]]
        faces = [euler_interface(row[at], row[at + 1], 0) for at in range(nx + 1)]
        for x in range(nx):
            node = x % 4
            start = 1.0 / WEIGHTS[0] if node == 0 else alpha[x] * float(1.0 / WEIGHTS[node])
            stop = 1.0 / WEIGHTS[3] if node == 3 else alpha[x] * float(1.0 / WEIGHTS[node])
            for var in range(5):
                total[var][x] += stop * faces[x + 1][var] - start * faces[x][var]
        column = [recv_z[0, side] for side in range(2)]
        for axis in range(2):
            for x in range(nx):
                start, stop = face_coefs(axis, alpha[x])
                halos = [
                    [
                        halo_y(0, side, var * nx + x)
                        if axis == 0
                        else halo_z(column[side], var * nx + x)
                        for var in range(5)
                    ]
                    for side in range(2)
                ]
                before = primitive(
                    [plane.previous(state[var][x], halos[0][var], axis) for var in range(5)]
                )
                after = primitive(
                    [plane.following(state[var][x], halos[1][var], axis) for var in range(5)]
                )
                left = euler_interface(before, nodes[x], axis + 1)
                right = euler_interface(nodes[x], after, axis + 1)
                for var in range(5):
                    total[var][x] += stop * right[var] - start * left[var]
        rate = [[-(2.0 / elem_width) * total[var][x] for x in range(nx)] for var in range(5)]
        for x in range(nx):
            for comp in range(3):
                rate[1 + comp][x] = rate[1 + comp][x] - state[0][x] * grav[1 + comp][x]
            rate[4][x] = rate[4][x] - (
                state[1][x] * grav[1][x] + state[2][x] * grav[2][x] + state[3][x] * grav[3][x]
            )
            for var in range(5):
                rate_ref[var, x] = rate[var][x]
        mass_rows = [weighted_row(rate[0])]
        reduce_start(1, 0, mass_rows)

        first_rows = reduce_finish(0, first_rows, [jnp.maximum, jnp.add])
        fastest = jnp.max(first_rows[0], axis=1, keepdims=True)
        mean_now = jnp.sum(first_rows[1], axis=1, keepdims=True) * (1.0 / weight_total)
        time_step = cfl_euler * elem_width / (7.0 * fastest)
        state_next = [
            [state[var][x] + time_step * rate[var][x] for x in range(nx)] for var in range(4)
        ]

        def gravity_rate(grav, round_at, offset):
            result = [
                [-coupling * (state_next[0][x] - offset) for x in range(nx)],
            ] + [[-grav[1 + comp][x] / relax_time for x in range(nx)] for comp in range(3)]
            scale = -(2.0 / elem_width)
            for start in range(0, nx, 4):
                for node in range(4):
                    for other in range(4):
                        coef = float(-scale * DERIV_FOLDED[node, other])
                        result[0][start + node] += coef * grav[1][start + other]
                        result[1][start + node] += coef / relax_time * grav[0][start + other]
            for axis in range(2):
                for x in range(nx):
                    matrix = -scale * DERIV_FOLDED
                    result[0][x] += plane.apply(matrix, grav[2 + axis][x], axis)
                    result[2 + axis][x] += plane.apply(matrix / relax_time, grav[0][x], axis)
            return result, scale

        def gravity_faces(result, scale, grav, round_at, first_at):
            edges = [[halo_xg[round_at, side, var] for var in range(4)] for side in range(2)]
            row = [edges[0]] + [[grav[var][x] for var in range(4)] for x in range(nx)] + [edges[1]]
            for x in range(0, nx, 4):
                left = gravity_interface(row[x], row[x + 1], 0)
                right = gravity_interface(row[x + 4], row[x + 5], 0)
                for var in range(4):
                    result[var][x] += float(-scale / WEIGHTS[0]) * left[var]
                    result[var][x + 3] += float(scale / WEIGHTS[3]) * right[var]
            column = [recv_z[round_at, side] for side in range(2)]
            for axis in range(2):
                start = plane.coef([-scale / WEIGHTS[0], 0.0, 0.0, 0.0], axis)
                stop = plane.coef([0.0, 0.0, 0.0, scale / WEIGHTS[3]], axis)
                for x in range(nx):
                    halos = [
                        [
                            halo_y(round_at, side, first_at + var * nx + x)
                            if axis == 0
                            else halo_z(column[side], first_at + var * nx + x)
                            for var in range(4)
                        ]
                        for side in range(2)
                    ]
                    here = [grav[var][x] for var in range(4)]
                    before = [plane.previous(here[var], halos[0][var], axis) for var in range(4)]
                    after = [plane.following(here[var], halos[1][var], axis) for var in range(4)]
                    left = gravity_interface(before, here, axis + 1)
                    right = gravity_interface(here, after, axis + 1)
                    for var in range(4):
                        result[var][x] += start * left[var] + stop * right[var]
            return result

        for iteration in range(ITERS):
            rate_grav, scale = gravity_rate(grav, iteration, mean_now)
            if iteration > 0:
                for copy in copies:
                    copy.wait()
            rate_grav = gravity_faces(
                rate_grav, scale, grav, iteration, 5 * nx if iteration == 0 else 0
            )
            if iteration < ITERS - 1:
                grav = [
                    [grav[var][x] + pseudo_step * rate_grav[var][x] for x in range(nx)]
                    for var in range(4)
                ]
                for var in range(4):
                    for x in range(nx):
                        grav_bufs[iteration + 1, var, x] = grav[var][x]
                pack(iteration + 1, grav)
                copies = exchange(iteration + 1)
        mass_rows = reduce_finish(1, mass_rows, [jnp.add])
        mean_more = time_step * (
            jnp.sum(mass_rows[0], axis=1, keepdims=True) * (1.0 / weight_total)
        )
        rate_phi = [item + coupling * mean_more for item in rate_grav[0]]
        norm_rows = [weighted_row([item * item for item in rate_phi])]
        reduce_start(2, 0, norm_rows)
        late = (ITERS - 1) * pseudo_step * coupling * mean_more
        rate_grav[0] = rate_phi
        grav = [
            [grav[var][x] + pseudo_step * rate_grav[var][x] for x in range(nx)] for var in range(4)
        ]
        for x in range(nx):
            grav[0][x] = grav[0][x] + late
            for var in range(4):
                grav_ref[var, x] = grav[var][x]
            for comp in range(3):
                source_ref[comp, x] = -state_next[0][x] * grav[1 + comp][x]
            source_ref[3, x] = -(
                state_next[1][x] * grav[1][x]
                + state_next[2][x] * grav[2][x]
                + state_next[3][x] * grav[3][x]
            )
        norm_rows = reduce_finish(2, norm_rows, [jnp.add])
        squared = jnp.sum(norm_rows[0], axis=1, keepdims=True)
        norm_ref[...] = jnp.sqrt(squared * (1.0 / weight_total))

    rows_y = 8 * ((9 * nx + 7) // 8)
    plane_shape = (ny, nz)
    scratch = [
        pltpu.VMEM((5, nx) + plane_shape, jnp.float32),
        pltpu.VMEM((ITERS, 4, nx) + plane_shape, jnp.float32),
        pltpu.VMEM((2, 5) + plane_shape, jnp.float32),
        pltpu.VMEM((ITERS, 2, 4) + plane_shape, jnp.float32),
        pltpu.VMEM((ITERS, 2, rows_y, nz), jnp.float32),
        pltpu.VMEM((ITERS, 2, rows_y, nz), jnp.float32),
        pltpu.VMEM((ITERS, 2) + plane_shape, jnp.float32),
        pltpu.VMEM((ITERS, 2) + plane_shape, jnp.float32),
        pltpu.VMEM((3, len(stages), 2, 1, nz), jnp.float32),
    ]
    for axes in stages:
        scratch.append(pltpu.VMEM((3, len(offsets_of(axes, sizes)), 2, 1, nz), jnp.float32))
    scratch += [
        pltpu.SemaphoreType.DMA((2,)),
        pltpu.SemaphoreType.DMA((ITERS, 8)),
        pltpu.SemaphoreType.DMA((ITERS, 8)),
        pltpu.SemaphoreType.DMA((3, len(stages))),
        pltpu.SemaphoreType.DMA((3, len(stages))),
    ]
    return kernel, scratch


def solution(mesh):
    sizes = {axis: mesh.shape[axis] for axis in AXES}

    def local(euler_state, gravity_state):
        shape = euler_state.shape[1:]
        kernel, scratch = make_kernel(sizes, shape)
        vmem = pl.BlockSpec(memory_space=pltpu.VMEM)
        rate, gravity, source, norm = pl.pallas_call(
            kernel,
            out_shape=(
                jax.ShapeDtypeStruct((5,) + shape, jnp.float32),
                jax.ShapeDtypeStruct((4,) + shape, jnp.float32),
                jax.ShapeDtypeStruct((4,) + shape, jnp.float32),
                jax.ShapeDtypeStruct((1, 1), jnp.float32),
            ),
            in_specs=[pl.BlockSpec(memory_space=pl.ANY)] * 2,
            out_specs=(vmem, vmem, vmem, vmem),
            scratch_shapes=scratch,
            compiler_params=pltpu.CompilerParams(collective_id=0, has_side_effects=True),
        )(euler_state, gravity_state)
        return rate, gravity, source, norm.reshape(())

    placed = (P(None, "gx", "gy", "gz"), P(None, "gx", "gy", "gz"))
    return jax.shard_map(
        local,
        mesh=mesh,
        in_specs=placed,
        out_specs=placed[:1] * 3 + (P(),),
        check_vma=False,
    )
```

```python
import itertools
import math

import jax
import jax.numpy as jnp
import numpy as np
from jax import lax
from jax.experimental import pallas as pl
from jax.experimental.pallas import tpu as pltpu
from jax.sharding import PartitionSpec as P

ITERS = 3
AXES = ("gx", "gy", "gz")
MOST_PARTNERS = 64

gamma_gas = 1.4
elem_width = 1.0
cfl_euler = 0.5
alpha_most = 0.5
indicator_level = 0.5 * 10.0 ** (-1.8 * 4.0**0.25)
indicator_slope = math.log((1.0 - 0.0001) / 0.0001) / indicator_level
coupling = 10.0
relax_time = 1.0
grav_speed = 1.0
pseudo_step = 0.3 * elem_width / 7.0
MESH = pl.DeviceIdType.MESH


def lgl_tables():
    points = np.array([-1.0, -1.0 / math.sqrt(5.0), 1.0 / math.sqrt(5.0), 1.0])
    weights = np.array([1.0, 5.0, 5.0, 1.0]) / 6.0
    barycentric = np.array(
        [
            1.0
            / np.prod([points[node_a] - points[node_b] for node_b in range(4) if node_b != node_a])
            for node_a in range(4)
        ]
    )
    derivative = np.zeros((4, 4))
    for node_a in range(4):
        for node_b in range(4):
            if node_b != node_a:
                derivative[node_a, node_b] = (
                    barycentric[node_b] / barycentric[node_a] / (points[node_a] - points[node_b])
                )
        derivative[node_a, node_a] = -np.sum(derivative[node_a])
    legendre = np.stack(
        [np.ones(4), points, 0.5 * (3.0 * points**2 - 1.0), 0.5 * (5.0 * points**3 - 3.0 * points)],
        axis=1,
    )
    legendre = legendre * np.sqrt((2.0 * np.arange(4) + 1.0) / 2.0)
    gram = np.sum(weights[:, None] * legendre * legendre, axis=0)
    modal_map = (legendre * weights[:, None]).T / gram[:, None]
    return (weights, derivative, modal_map)


WEIGHTS, DERIV, MODAL = lgl_tables()
DERIV_FOLDED = DERIV.copy()
DERIV_FOLDED[0, 0] += 1.0 / WEIGHTS[0]
DERIV_FOLDED[3, 3] -= 1.0 / WEIGHTS[3]
SELF_COEF = 2.0 * np.diag(DERIV)
SELF_COEF[0] += 1.0 / WEIGHTS[0]
SELF_COEF[3] -= 1.0 / WEIGHTS[3]


def reduce_stages(sizes):
    total = math.prod(sizes[axis] for axis in AXES)
    if total <= MOST_PARTNERS:
        return [AXES]
    return [("gx", "gy"), ("gz",)]


def offsets_of(axes, sizes):
    ranges = [range(sizes[axis]) for axis in axes]
    return [item for item in itertools.product(*ranges) if any(item)]


class Plane:
    def __init__(self, ny, nz):
        self.shape = (ny, nz)
        self.index = [lax.broadcasted_iota(jnp.int32, (ny, nz), axis) for axis in range(2)]
        self.node = [item & 3 for item in self.index]
        self.is_node = [[node == value for value in range(4)] for node in self.node]
        self.cache = {}

    def coef(self, values, axis):
        values = tuple(float(np.float32(value)) for value in values)
        if len(set(values)) == 1:
            return values[0]
        key = (values, axis)
        if key not in self.cache:
            result = jnp.full(self.shape, values[3], jnp.float32)
            for node in range(2, -1, -1):
                result = jnp.where(self.is_node[axis][node], values[node], result)
            self.cache[key] = result
        return self.cache[key]

    def ahead(self, value, by, axis):
        return pltpu.roll(value, (-by) % self.shape[axis], axis)

    def apply(self, matrix, value, axis):
        total = self.coef(np.diag(matrix), axis) * value
        for by in range(1, 4):
            up = [matrix[node, node + by] if node + by < 4 else 0.0 for node in range(4)]
            down = [matrix[node, node - by] if node - by >= 0 else 0.0 for node in range(4)]
            total = total + self.coef(up, axis) * self.ahead(value, by, axis)
            total = total + self.coef(down, axis) * self.ahead(value, -by, axis)
        return total

    def previous(self, value, halo, axis):
        return jnp.where(self.index[axis] == 0, halo, self.ahead(value, -1, axis))

    def following(self, value, halo, axis):
        last = self.shape[axis] - 1
        return jnp.where(self.index[axis] == last, halo, self.ahead(value, 1, axis))


def primitive(state):
    inverse = 1.0 / state[0]
    vel = [state[1 + comp] * inverse for comp in range(3)]
    kinetic = state[1] * vel[0] + state[2] * vel[1] + state[3] * vel[2]
    pressure = (gamma_gas - 1.0) * (state[4] - 0.5 * kinetic)
    sound = jnp.sqrt(gamma_gas * pressure * inverse)
    return list(state) + vel + [pressure, sound]


def flux_of(node, direction):
    normal = node[5 + direction]
    momentum = [
        node[1 + comp] * normal + node[8] if comp == direction else node[1 + comp] * normal
        for comp in range(3)
    ]
    return [node[1 + direction]] + momentum + [(node[4] + node[8]) * normal]


def euler_interface(left, right, direction):
    speed = 0.5 * jnp.maximum(
        jnp.abs(left[5 + direction]) + left[9], jnp.abs(right[5 + direction]) + right[9]
    )
    flux_left, flux_right = flux_of(left, direction), flux_of(right, direction)
    return [
        0.5 * (flux_left[var] + flux_right[var]) - speed * (right[var] - left[var])
        for var in range(5)
    ]


def log_mean_parts(left, right):
    total = left + right
    ratio = (left - right) / total
    ratio_sq = ratio * ratio
    is_close = ratio_sq < 0.0001
    series = 2.0 + ratio_sq * (2.0 / 3.0 + ratio_sq * (2.0 / 5.0 + ratio_sq * (2.0 / 7.0)))
    top = jnp.where(is_close, total, right - left)
    low = jnp.where(is_close, series, jnp.log(right / left))
    return top, low


def two_point(left, right, direction):
    top, low = log_mean_parts(left[0], right[0])
    rho_mean = top / low
    top, low = log_mean_parts(left[0] * right[4], right[0] * left[4])
    inv_mean = left[4] * right[4] * low / top
    vel_avg = [0.5 * (left[1 + comp] + right[1 + comp]) for comp in range(3)]
    pres_avg = 0.5 * (left[4] + right[4])
    vel_product = 0.5 * (left[1] * right[1] + left[2] * right[2] + left[3] * right[3])
    mass = rho_mean * vel_avg[direction]
    momentum = [
        mass * vel_avg[comp] + pres_avg if comp == direction else mass * vel_avg[comp]
        for comp in range(3)
    ]
    energy = mass * (vel_product + inv_mean * (1.0 / (gamma_gas - 1.0))) + 0.5 * (
        left[4] * right[1 + direction] + right[4] * left[1 + direction]
    )
    return [mass] + momentum + [energy]


def gravity_interface(left, right, direction):
    result = []
    for var in range(4):
        jump = 0.5 * grav_speed * (right[var] - left[var])
        if var == 0:
            result.append(-0.5 * (left[1 + direction] + right[1 + direction]) - jump)
        elif var == 1 + direction:
            result.append(-(0.5 / relax_time) * (left[0] + right[0]) - jump)
        else:
            result.append(-jump)
    return result


def add_volume(volume, nodes, plane, nx):
    pair_fields = [[node[0], node[5], node[6], node[7], node[8]] for node in nodes]

    def add(x, terms):
        for var in range(5):
            old = volume[var][x]
            volume[var][x] = terms[var] if old is None else old + terms[var]

    for start in range(0, nx, 4):
        for low in range(4):
            own = flux_of(nodes[start + low], 0)
            coef = float(np.float32(SELF_COEF[low]))
            add(start + low, [coef * item for item in own])
            for high in range(low + 1, 4):
                flux = two_point(pair_fields[start + low], pair_fields[start + high], 0)
                add(start + low, [float(2.0 * DERIV[low, high]) * item for item in flux])
                add(start + high, [float(2.0 * DERIV[high, low]) * item for item in flux])
    deriv = 2.0 * DERIV
    for axis in range(2):
        direction = axis + 1
        for x in range(nx):
            here = pair_fields[x]
            own = flux_of(nodes[x], direction)
            coef = plane.coef(SELF_COEF, axis)
            add(x, [coef * item for item in own])
            there = [plane.ahead(item, 1, axis) for item in here]
            flux = two_point(here, there, direction)
            up = plane.coef([deriv[0, 1], deriv[1, 2], deriv[2, 3], 0.0], axis)
            down = plane.coef([0.0, deriv[1, 0], deriv[2, 1], deriv[3, 2]], axis)
            add(x, [up * item + down * plane.ahead(item, -1, axis) for item in flux])
            is_last = plane.is_node[axis][3]
            there = [
                jnp.where(is_last, plane.ahead(item, -3, axis), plane.ahead(item, 2, axis))
                for item in here
            ]
            flux = two_point(here, there, direction)
            own_coef = plane.coef([deriv[0, 2], deriv[1, 3], 0.0, deriv[3, 0]], axis)
            down = plane.coef([0.0, 0.0, deriv[2, 0], deriv[3, 1]], axis)
            up = plane.coef([deriv[0, 3], 0.0, 0.0, 0.0], axis)
            add(
                x,
                [
                    own_coef * item
                    + down * plane.ahead(item, -2, axis)
                    + up * plane.ahead(item, 3, axis)
                    for item in flux
                ],
            )


def element_alpha(nodes, plane, nx):
    ones = np.ones((4, 4))
    low_index = np.array([1.0, 1.0, 1.0, 0.0])
    not_low = 1.0 - plane.coef(low_index, 0) * plane.coef(low_index, 1)
    result = []
    for start in range(0, nx, 4):
        product = [nodes[start + node][0] * nodes[start + node][8] for node in range(4)]
        energies = []
        for mode in range(4):
            coeffs = sum(float(MODAL[mode, node]) * product[node] for node in range(4))
            coeffs = plane.apply(MODAL, plane.apply(MODAL, coeffs, 0), 1)
            energies.append(coeffs * coeffs)
        low_part = energies[0] + energies[1] + energies[2]
        sums = [low_part + energies[3], low_part * not_low + energies[3]]
        sums = [plane.apply(ones, plane.apply(ones, item, 1), 0) for item in sums]
        share = sums[1] / sums[0]
        alpha = alpha_most / (1.0 + jnp.exp(-indicator_slope * (share - indicator_level)))
        result += [alpha] * 4
    return result


def make_kernel(sizes, shape):
    nx, ny, nz = shape
    stages = reduce_stages(sizes)
    weight_total = (
        8.0 * (nx // 4) * (ny // 4) * (nz // 4) * math.prod(sizes[axis] for axis in AXES)
    )

    def kernel(
        euler_hbm,
        gravity_hbm,
        rate_ref,
        grav_ref,
        source_ref,
        norm_ref,
        euler_ref,
        grav_bufs,
        halo_xe,
        halo_xg,
        send_y,
        recv_y,
        send_z,
        recv_z,
        reduce_send,
        *rest,
    ):
        reduce_recv = rest[: len(stages)]
        load_sem, send_sem, recv_sem, reduce_send_sem, reduce_recv_sem = rest[len(stages) :]
        place = {axis: lax.axis_index(axis) for axis in AXES}

        def moved(axis, by):
            size = sizes[axis]
            by = by % size
            if by == 0:
                return place[axis]
            target = place[axis] + by
            return jnp.where(target >= size, target - size, target)

        targets = {axis: [moved(axis, by) for by in range(sizes[axis])] for axis in AXES}

        def device(axes, offset):
            return {axis: targets[axis][by] for axis, by in zip(axes, offset)}

        barrier = pltpu.get_barrier_semaphore()
        count = 0
        for axes in stages:
            for offset in offsets_of(axes, sizes):
                pl.semaphore_signal(
                    barrier, inc=1, device_id=device(axes, offset), device_id_type=MESH
                )
                count += 1
        load_euler = pltpu.make_async_copy(euler_hbm, euler_ref, load_sem.at[0])
        load_gravity = pltpu.make_async_copy(gravity_hbm, grav_bufs.at[0], load_sem.at[1])
        load_euler.start()
        load_gravity.start()
        load_euler.wait()
        load_gravity.wait()

        plane = Plane(ny, nz)
        state = [[euler_ref[var, x] for x in range(nx)] for var in range(5)]
        grav = [[grav_bufs[0, var, x] for x in range(nx)] for var in range(4)]

        def pack(round_at, fields):
            lanes = [jnp.zeros((ny, nz), jnp.float32) for side in range(2)]
            for at, item in enumerate(itertools.chain(*fields)):
                send_y[round_at, 0, at : at + 1, :] = item[ny - 1 : ny, :]
                send_y[round_at, 1, at : at + 1, :] = item[0:1, :]
                here = plane.index[1] == at
                lanes[0] = jnp.where(here, plane.ahead(item, nz - 1 - at, 1), lanes[0])
                lanes[1] = jnp.where(here, plane.ahead(item, -at, 1), lanes[1])
            send_z[round_at, 0] = lanes[0]
            send_z[round_at, 1] = lanes[1]

        def exchange(round_at):
            copies = []

            def send(src, dst, slot, axis, by):
                copy = pltpu.make_async_remote_copy(
                    src_ref=src,
                    dst_ref=dst,
                    send_sem=send_sem.at[round_at, slot],
                    recv_sem=recv_sem.at[round_at, slot],
                    device_id=device((axis,), (by % sizes[axis],)),
                    device_id_type=MESH,
                )
                copy.start()
                copies.append(copy)

            for side, by in ((0, 1), (1, -1)):
                face = nx - 1 if side == 0 else 0
                if round_at == 0:
                    send(euler_ref.at[:, face], halo_xe.at[side], 6 + side, "gx", by)
                send(
                    grav_bufs.at[round_at, :, face], halo_xg.at[round_at, side], side, "gx", by
                )
                rows = recv_y.shape[2] if round_at == 0 else 8 * ((4 * nx + 7) // 8)
                send(
                    send_y.at[round_at, side, pl.ds(0, rows)],
                    recv_y.at[round_at, side, pl.ds(0, rows)],
                    2 + side,
                    "gy",
                    by,
                )
                send(send_z.at[round_at, side], recv_z.at[round_at, side], 4 + side, "gz", by)
            return copies

        def halo_y(round_at, side, at):
            return jnp.broadcast_to(recv_y[round_at, side, at : at + 1, :], (ny, nz))

        def halo_z(column, at):
            return jnp.broadcast_to(column[:, at : at + 1], (ny, nz))

        def reduce_start(round_at, stage_at, rows):
            axes = stages[stage_at]
            for at, row in enumerate(rows):
                reduce_send[round_at, stage_at, at] = row
            copies = []
            for slot, offset in enumerate(offsets_of(axes, sizes)):
                copy = pltpu.make_async_remote_copy(
                    src_ref=reduce_send.at[round_at, stage_at, pl.ds(0, len(rows))],
                    dst_ref=reduce_recv[stage_at].at[round_at, slot, pl.ds(0, len(rows))],
                    send_sem=reduce_send_sem.at[round_at, stage_at],
                    recv_sem=reduce_recv_sem.at[round_at, stage_at],
                    device_id=device(axes, offset),
                    device_id_type=MESH,
                )
                copy.start()

        def reduce_finish(round_at, rows, combine):
            for stage_at in range(len(stages)):
                if stage_at > 0:
                    reduce_start(round_at, stage_at, rows)
                got = reduce_recv[stage_at].at[round_at, :, pl.ds(0, len(rows))]
                pltpu.make_async_copy(got, got, reduce_recv_sem.at[round_at, stage_at]).wait()
                pltpu.make_async_copy(got, got, reduce_send_sem.at[round_at, stage_at]).wait()
                partners = reduce_recv[stage_at].shape[1]
                new_rows = []
                for at, row in enumerate(rows):
                    parts = [row] + [
                        reduce_recv[stage_at][round_at, slot, at] for slot in range(partners)
                    ]
                    while len(parts) > 1:
                        pairs = [
                            combine[at](parts[item], parts[item + 1])
                            for item in range(0, len(parts) - 1, 2)
                        ]
                        parts = pairs + ([parts[-1]] if len(parts) % 2 else [])
                    new_rows.append(parts[0])
                rows = new_rows
            return rows

        pack(0, state + grav)
        nodes = [primitive([state[var][x] for var in range(5)]) for x in range(nx)]
        weight_yz = plane.coef(WEIGHTS, 0) * plane.coef(WEIGHTS, 1)

        def weighted_row(items):
            total = sum(float(WEIGHTS[x % 4]) * items[x] for x in range(nx))
            return jnp.sum(weight_yz * total, axis=0, keepdims=True)

        speeds = [
            jnp.abs(node[5]) + jnp.abs(node[6]) + jnp.abs(node[7]) + 3.0 * node[9] for node in nodes
        ]
        fastest = speeds[0]
        for item in speeds[1:]:
            fastest = jnp.maximum(fastest, item)
        first_rows = [jnp.max(fastest, axis=0, keepdims=True), weighted_row(state[0])]

        pl.semaphore_wait(barrier, count)
        copies_0 = exchange(0)
        reduce_start(0, 0, first_rows)

        alpha = element_alpha(nodes, plane, nx)
        volume = [[None] * nx for var in range(5)]
        add_volume(volume, nodes, plane, nx)
        total = [[(1.0 - alpha[x]) * volume[var][x] for x in range(nx)] for var in range(5)]

        for copy in copies_0:
            copy.wait()

        def face_coefs(axis, alpha_x):
            start = jnp.where(plane.is_node[axis][0], 1.0, alpha_x)
            stop = jnp.where(plane.is_node[axis][3], 1.0, alpha_x)
            inverse = plane.coef(1.0 / WEIGHTS, axis)
            return start * inverse, stop * inverse

        edges = [primitive([halo_xe[side, var] for var in range(5)]) for side in range(2)]
        row = [edges[0]] + nodes + [edges[1]]
        faces = [euler_interface(row[at], row[at + 1], 0) for at in range(nx + 1)]
        for x in range(nx):
            node = x % 4
            start = 1.0 / WEIGHTS[0] if node == 0 else alpha[x] * float(1.0 / WEIGHTS[node])
            stop = 1.0 / WEIGHTS[3] if node == 3 else alpha[x] * float(1.0 / WEIGHTS[node])
            for var in range(5):
                total[var][x] += stop * faces[x + 1][var] - start * faces[x][var]
        column = [recv_z[0, side] for side in range(2)]
        for axis in range(2):
            for x in range(nx):
                start, stop = face_coefs(axis, alpha[x])
                halos = [
                    [
                        halo_y(0, side, var * nx + x)
                        if axis == 0
                        else halo_z(column[side], var * nx + x)
                        for var in range(5)
                    ]
                    for side in range(2)
                ]
                before = primitive(
                    [plane.previous(state[var][x], halos[0][var], axis) for var in range(5)]
                )
                after = primitive(
                    [plane.following(state[var][x], halos[1][var], axis) for var in range(5)]
                )
                left = euler_interface(before, nodes[x], axis + 1)
                right = euler_interface(nodes[x], after, axis + 1)
                for var in range(5):
                    total[var][x] += stop * right[var] - start * left[var]
        rate = [[-(2.0 / elem_width) * total[var][x] for x in range(nx)] for var in range(5)]
        for x in range(nx):
            for comp in range(3):
                rate[1 + comp][x] = rate[1 + comp][x] - state[0][x] * grav[1 + comp][x]
            rate[4][x] = rate[4][x] - (
                state[1][x] * grav[1][x] + state[2][x] * grav[2][x] + state[3][x] * grav[3][x]
            )
            for var in range(5):
                rate_ref[var, x] = rate[var][x]
        mass_rows = [weighted_row(rate[0])]
        reduce_start(1, 0, mass_rows)

        first_rows = reduce_finish(0, first_rows, [jnp.maximum, jnp.add])
        fastest = jnp.max(first_rows[0], axis=1, keepdims=True)
        mean_now = jnp.sum(first_rows[1], axis=1, keepdims=True) * (1.0 / weight_total)
        time_step = cfl_euler * elem_width / (7.0 * fastest)
        state_next = [
            [state[var][x] + time_step * rate[var][x] for x in range(nx)] for var in range(4)
        ]

        def gravity_rate(grav, round_at, offset):
            result = [
                [-coupling * (state_next[0][x] - offset) for x in range(nx)],
            ] + [[-grav[1 + comp][x] / relax_time for x in range(nx)] for comp in range(3)]
            scale = -(2.0 / elem_width)
            for start in range(0, nx, 4):
                for node in range(4):
                    for other in range(4):
                        coef = float(-scale * DERIV_FOLDED[node, other])
                        result[0][start + node] += coef * grav[1][start + other]
                        result[1][start + node] += coef / relax_time * grav[0][start + other]
            for axis in range(2):
                for x in range(nx):
                    matrix = -scale * DERIV_FOLDED
                    result[0][x] += plane.apply(matrix, grav[2 + axis][x], axis)
                    result[2 + axis][x] += plane.apply(matrix / relax_time, grav[0][x], axis)
            return result, scale

        def gravity_faces(result, scale, grav, round_at, first_at):
            edges = [[halo_xg[round_at, side, var] for var in range(4)] for side in range(2)]
            row = [edges[0]] + [[grav[var][x] for var in range(4)] for x in range(nx)] + [edges[1]]
            for x in range(0, nx, 4):
                left = gravity_interface(row[x], row[x + 1], 0)
                right = gravity_interface(row[x + 4], row[x + 5], 0)
                for var in range(4):
                    result[var][x] += float(-scale / WEIGHTS[0]) * left[var]
                    result[var][x + 3] += float(scale / WEIGHTS[3]) * right[var]
            column = [recv_z[round_at, side] for side in range(2)]
            for axis in range(2):
                start = plane.coef([-scale / WEIGHTS[0], 0.0, 0.0, 0.0], axis)
                stop = plane.coef([0.0, 0.0, 0.0, scale / WEIGHTS[3]], axis)
                for x in range(nx):
                    halos = [
                        [
                            halo_y(round_at, side, first_at + var * nx + x)
                            if axis == 0
                            else halo_z(column[side], first_at + var * nx + x)
                            for var in range(4)
                        ]
                        for side in range(2)
                    ]
                    here = [grav[var][x] for var in range(4)]
                    before = [plane.previous(here[var], halos[0][var], axis) for var in range(4)]
                    after = [plane.following(here[var], halos[1][var], axis) for var in range(4)]
                    left = gravity_interface(before, here, axis + 1)
                    right = gravity_interface(here, after, axis + 1)
                    for var in range(4):
                        result[var][x] += start * left[var] + stop * right[var]
            return result

        for iteration in range(ITERS):
            rate_grav, scale = gravity_rate(grav, iteration, mean_now)
            if iteration > 0:
                for copy in copies:
                    copy.wait()
            rate_grav = gravity_faces(
                rate_grav, scale, grav, iteration, 5 * nx if iteration == 0 else 0
            )
            if iteration < ITERS - 1:
                grav = [
                    [grav[var][x] + pseudo_step * rate_grav[var][x] for x in range(nx)]
                    for var in range(4)
                ]
                for var in range(4):
                    for x in range(nx):
                        grav_bufs[iteration + 1, var, x] = grav[var][x]
                pack(iteration + 1, grav)
                copies = exchange(iteration + 1)
        mass_rows = reduce_finish(1, mass_rows, [jnp.add])
        mean_more = time_step * (
            jnp.sum(mass_rows[0], axis=1, keepdims=True) * (1.0 / weight_total)
        )
        rate_phi = [item + coupling * mean_more for item in rate_grav[0]]
        norm_rows = [weighted_row([item * item for item in rate_phi])]
        reduce_start(2, 0, norm_rows)
        late = (ITERS - 1) * pseudo_step * coupling * mean_more
        rate_grav[0] = rate_phi
        grav = [
            [grav[var][x] + pseudo_step * rate_grav[var][x] for x in range(nx)] for var in range(4)
        ]
        for x in range(nx):
            grav[0][x] = grav[0][x] + late
            for var in range(4):
                grav_ref[var, x] = grav[var][x]
            for comp in range(3):
                source_ref[comp, x] = -state_next[0][x] * grav[1 + comp][x]
            source_ref[3, x] = -(
                state_next[1][x] * grav[1][x]
                + state_next[2][x] * grav[2][x]
                + state_next[3][x] * grav[3][x]
            )
        norm_rows = reduce_finish(2, norm_rows, [jnp.add])
        squared = jnp.sum(norm_rows[0], axis=1, keepdims=True)
        norm_ref[...] = jnp.sqrt(squared * (1.0 / weight_total))

    rows_y = 8 * ((9 * nx + 7) // 8)
    plane_shape = (ny, nz)
    scratch = [
        pltpu.VMEM((5, nx) + plane_shape, jnp.float32),
        pltpu.VMEM((ITERS, 4, nx) + plane_shape, jnp.float32),
        pltpu.VMEM((2, 5) + plane_shape, jnp.float32),
        pltpu.VMEM((ITERS, 2, 4) + plane_shape, jnp.float32),
        pltpu.VMEM((ITERS, 2, rows_y, nz), jnp.float32),
        pltpu.VMEM((ITERS, 2, rows_y, nz), jnp.float32),
        pltpu.VMEM((ITERS, 2) + plane_shape, jnp.float32),
        pltpu.VMEM((ITERS, 2) + plane_shape, jnp.float32),
        pltpu.VMEM((3, len(stages), 2, 1, nz), jnp.float32),
    ]
    for axes in stages:
        scratch.append(pltpu.VMEM((3, len(offsets_of(axes, sizes)), 2, 1, nz), jnp.float32))
    scratch += [
        pltpu.SemaphoreType.DMA((2,)),
        pltpu.SemaphoreType.DMA((ITERS, 8)),
        pltpu.SemaphoreType.DMA((ITERS, 8)),
        pltpu.SemaphoreType.DMA((3, len(stages))),
        pltpu.SemaphoreType.DMA((3, len(stages))),
    ]
    return kernel, scratch


def solution(mesh):
    sizes = {axis: mesh.shape[axis] for axis in AXES}

    def local(euler_state, gravity_state):
        shape = euler_state.shape[1:]
        kernel, scratch = make_kernel(sizes, shape)
        vmem = pl.BlockSpec(memory_space=pltpu.VMEM)
        rate, gravity, source, norm = pl.pallas_call(
            kernel,
            out_shape=(
                pltpu.VMEM((5,) + shape, jnp.float32),
                pltpu.VMEM((4,) + shape, jnp.float32),
                pltpu.VMEM((4,) + shape, jnp.float32),
                jax.ShapeDtypeStruct((1, 1), jnp.float32),
            ),
            in_specs=[pl.BlockSpec(memory_space=pl.ANY)] * 2,
            out_specs=(vmem, vmem, vmem, vmem),
            scratch_shapes=scratch,
            compiler_params=pltpu.CompilerParams(collective_id=0, has_side_effects=True),
        )(euler_state, gravity_state)
        return rate, gravity, source, norm.reshape(())

    placed = (P(None, "gx", "gy", "gz"), P(None, "gx", "gy", "gz"))
    return jax.shard_map(
        local,
        mesh=mesh,
        in_specs=placed,
        out_specs=placed[:1] * 3 + (P(),),
        check_vma=False,
    )
```

```python
import itertools
import math

import jax
import jax.numpy as jnp
import numpy as np
from jax import lax
from jax.experimental import pallas as pl
from jax.experimental.pallas import tpu as pltpu
from jax.sharding import PartitionSpec as P

ITERS = 3
AXES = ("gx", "gy", "gz")
MOST_PARTNERS = 64

gamma_gas = 1.4
elem_width = 1.0
cfl_euler = 0.5
alpha_most = 0.5
indicator_level = 0.5 * 10.0 ** (-1.8 * 4.0**0.25)
indicator_slope = math.log((1.0 - 0.0001) / 0.0001) / indicator_level
coupling = 10.0
relax_time = 1.0
grav_speed = 1.0
pseudo_step = 0.3 * elem_width / 7.0
MESH = pl.DeviceIdType.MESH


def lgl_tables():
    points = np.array([-1.0, -1.0 / math.sqrt(5.0), 1.0 / math.sqrt(5.0), 1.0])
    weights = np.array([1.0, 5.0, 5.0, 1.0]) / 6.0
    barycentric = np.array(
        [
            1.0
            / np.prod([points[node_a] - points[node_b] for node_b in range(4) if node_b != node_a])
            for node_a in range(4)
        ]
    )
    derivative = np.zeros((4, 4))
    for node_a in range(4):
        for node_b in range(4):
            if node_b != node_a:
                derivative[node_a, node_b] = (
                    barycentric[node_b] / barycentric[node_a] / (points[node_a] - points[node_b])
                )
        derivative[node_a, node_a] = -np.sum(derivative[node_a])
    legendre = np.stack(
        [np.ones(4), points, 0.5 * (3.0 * points**2 - 1.0), 0.5 * (5.0 * points**3 - 3.0 * points)],
        axis=1,
    )
    legendre = legendre * np.sqrt((2.0 * np.arange(4) + 1.0) / 2.0)
    gram = np.sum(weights[:, None] * legendre * legendre, axis=0)
    modal_map = (legendre * weights[:, None]).T / gram[:, None]
    return (weights, derivative, modal_map)


WEIGHTS, DERIV, MODAL = lgl_tables()
DERIV_FOLDED = DERIV.copy()
DERIV_FOLDED[0, 0] += 1.0 / WEIGHTS[0]
DERIV_FOLDED[3, 3] -= 1.0 / WEIGHTS[3]
SELF_COEF = 2.0 * np.diag(DERIV)
SELF_COEF[0] += 1.0 / WEIGHTS[0]
SELF_COEF[3] -= 1.0 / WEIGHTS[3]


def reduce_stages(sizes):
    lines = [(axis,) for axis in AXES]
    total = math.prod(sizes[axis] for axis in AXES)
    return [lines, [AXES] if total <= MOST_PARTNERS else lines]


def offsets_of(axes, sizes):
    ranges = [range(sizes[axis]) for axis in axes]
    return [item for item in itertools.product(*ranges) if any(item)]


class Plane:
    def __init__(self, ny, nz):
        self.shape = (ny, nz)
        self.index = [lax.broadcasted_iota(jnp.int32, (ny, nz), axis) for axis in range(2)]
        self.node = [item & 3 for item in self.index]
        self.is_node = [[node == value for value in range(4)] for node in self.node]
        self.cache = {}

    def coef(self, values, axis):
        values = tuple(float(np.float32(value)) for value in values)
        if len(set(values)) == 1:
            return values[0]
        key = (values, axis)
        if key not in self.cache:
            result = jnp.full(self.shape, values[3], jnp.float32)
            for node in range(2, -1, -1):
                result = jnp.where(self.is_node[axis][node], values[node], result)
            self.cache[key] = result
        return self.cache[key]

    def ahead(self, value, by, axis):
        return pltpu.roll(value, (-by) % self.shape[axis], axis)

    def apply(self, matrix, value, axis):
        total = self.coef(np.diag(matrix), axis) * value
        for by in range(1, 4):
            up = [matrix[node, node + by] if node + by < 4 else 0.0 for node in range(4)]
            down = [matrix[node, node - by] if node - by >= 0 else 0.0 for node in range(4)]
            total = total + self.coef(up, axis) * self.ahead(value, by, axis)
            total = total + self.coef(down, axis) * self.ahead(value, -by, axis)
        return total

    def previous(self, value, halo, axis):
        return jnp.where(self.index[axis] == 0, halo, self.ahead(value, -1, axis))

    def following(self, value, halo, axis):
        last = self.shape[axis] - 1
        return jnp.where(self.index[axis] == last, halo, self.ahead(value, 1, axis))


def primitive(state):
    inverse = 1.0 / state[0]
    vel = [state[1 + comp] * inverse for comp in range(3)]
    kinetic = state[1] * vel[0] + state[2] * vel[1] + state[3] * vel[2]
    pressure = (gamma_gas - 1.0) * (state[4] - 0.5 * kinetic)
    sound = jnp.sqrt(gamma_gas * pressure * inverse)
    return list(state) + vel + [pressure, sound]


def flux_of(node, direction):
    normal = node[5 + direction]
    momentum = [
        node[1 + comp] * normal + node[8] if comp == direction else node[1 + comp] * normal
        for comp in range(3)
    ]
    return [node[1 + direction]] + momentum + [(node[4] + node[8]) * normal]


def euler_interface(left, right, direction):
    speed = 0.5 * jnp.maximum(
        jnp.abs(left[5 + direction]) + left[9], jnp.abs(right[5 + direction]) + right[9]
    )
    flux_left, flux_right = flux_of(left, direction), flux_of(right, direction)
    return [
        0.5 * (flux_left[var] + flux_right[var]) - speed * (right[var] - left[var])
        for var in range(5)
    ]


def log_mean_parts(left, right):
    total = left + right
    ratio = (left - right) / total
    ratio_sq = ratio * ratio
    is_close = ratio_sq < 0.0001
    series = 2.0 + ratio_sq * (2.0 / 3.0 + ratio_sq * (2.0 / 5.0 + ratio_sq * (2.0 / 7.0)))
    top = jnp.where(is_close, total, right - left)
    low = jnp.where(is_close, series, jnp.log(right / left))
    return top, low


def two_point(left, right, direction):
    top, low = log_mean_parts(left[0], right[0])
    rho_mean = top / low
    top, low = log_mean_parts(left[0] * right[4], right[0] * left[4])
    inv_mean = left[4] * right[4] * low / top
    vel_avg = [0.5 * (left[1 + comp] + right[1 + comp]) for comp in range(3)]
    pres_avg = 0.5 * (left[4] + right[4])
    vel_product = 0.5 * (left[1] * right[1] + left[2] * right[2] + left[3] * right[3])
    mass = rho_mean * vel_avg[direction]
    momentum = [
        mass * vel_avg[comp] + pres_avg if comp == direction else mass * vel_avg[comp]
        for comp in range(3)
    ]
    energy = mass * (vel_product + inv_mean * (1.0 / (gamma_gas - 1.0))) + 0.5 * (
        left[4] * right[1 + direction] + right[4] * left[1 + direction]
    )
    return [mass] + momentum + [energy]


def gravity_interface(left, right, direction):
    result = []
    for var in range(4):
        parts = []
        other = 1 + direction if var == 0 else 0
        if var in (0, 1 + direction) and left[other] is not None:
            parts.append(-(0.5 / relax_time if var else 0.5) * (left[other] + right[other]))
        if left[var] is not None:
            parts.append((-0.5 * grav_speed) * (right[var] - left[var]))
        result.append(sum(parts[1:], parts[0]) if parts else None)
    return result


def add_volume(volume, nodes, plane, nx):
    pair_fields = [[node[0], node[5], node[6], node[7], node[8]] for node in nodes]

    def add(x, terms):
        for var in range(5):
            old = volume[var][x]
            volume[var][x] = terms[var] if old is None else old + terms[var]

    for start in range(0, nx, 4):
        for low in range(4):
            own = flux_of(nodes[start + low], 0)
            coef = float(np.float32(SELF_COEF[low]))
            add(start + low, [coef * item for item in own])
            for high in range(low + 1, 4):
                flux = two_point(pair_fields[start + low], pair_fields[start + high], 0)
                add(start + low, [float(2.0 * DERIV[low, high]) * item for item in flux])
                add(start + high, [float(2.0 * DERIV[high, low]) * item for item in flux])
    deriv = 2.0 * DERIV
    for axis in range(2):
        direction = axis + 1
        for x in range(nx):
            here = pair_fields[x]
            own = flux_of(nodes[x], direction)
            coef = plane.coef(SELF_COEF, axis)
            add(x, [coef * item for item in own])
            there = [plane.ahead(item, 1, axis) for item in here]
            flux = two_point(here, there, direction)
            up = plane.coef([deriv[0, 1], deriv[1, 2], deriv[2, 3], 0.0], axis)
            down = plane.coef([0.0, deriv[1, 0], deriv[2, 1], deriv[3, 2]], axis)
            add(x, [up * item + down * plane.ahead(item, -1, axis) for item in flux])
            is_last = plane.is_node[axis][3]
            there = [
                jnp.where(is_last, plane.ahead(item, -3, axis), plane.ahead(item, 2, axis))
                for item in here
            ]
            flux = two_point(here, there, direction)
            own_coef = plane.coef([deriv[0, 2], deriv[1, 3], 0.0, deriv[3, 0]], axis)
            down = plane.coef([0.0, 0.0, deriv[2, 0], deriv[3, 1]], axis)
            up = plane.coef([deriv[0, 3], 0.0, 0.0, 0.0], axis)
            add(
                x,
                [
                    own_coef * item
                    + down * plane.ahead(item, -2, axis)
                    + up * plane.ahead(item, 3, axis)
                    for item in flux
                ],
            )


def element_alpha(nodes, plane, nx):
    ones = np.ones((4, 4))
    low_index = np.array([1.0, 1.0, 1.0, 0.0])
    not_low = 1.0 - plane.coef(low_index, 0) * plane.coef(low_index, 1)
    result = []
    for start in range(0, nx, 4):
        product = [nodes[start + node][0] * nodes[start + node][8] for node in range(4)]
        energies = []
        for mode in range(4):
            coeffs = sum(float(MODAL[mode, node]) * product[node] for node in range(4))
            coeffs = plane.apply(MODAL, plane.apply(MODAL, coeffs, 0), 1)
            energies.append(coeffs * coeffs)
        low_part = energies[0] + energies[1] + energies[2]
        sums = [low_part + energies[3], low_part * not_low + energies[3]]
        sums = [plane.apply(ones, plane.apply(ones, item, 1), 0) for item in sums]
        share = sums[1] / sums[0]
        alpha = alpha_most / (1.0 + jnp.exp(-indicator_slope * (share - indicator_level)))
        result += [alpha] * 4
    return result


def make_kernel(sizes, shape):
    nx, ny, nz = shape
    stages = reduce_stages(sizes)
    weight_total = (
        8.0 * (nx // 4) * (ny // 4) * (nz // 4) * math.prod(sizes[axis] for axis in AXES)
    )

    def kernel(
        euler_hbm,
        gravity_hbm,
        rate_ref,
        grav_ref,
        source_ref,
        norm_ref,
        euler_ref,
        grav_bufs,
        halo_xe,
        halo_xg,
        send_y,
        recv_y,
        send_z,
        recv_z,
        reduce_send,
        *rest,
    ):
        reduce_recv = [rest[: len(stages[0])], rest[len(stages[0]) : -5]]
        load_sem, send_sem, recv_sem, reduce_send_sem, reduce_recv_sem = rest[-5:]
        place = {axis: lax.axis_index(axis) for axis in AXES}

        def moved(axis, by):
            size = sizes[axis]
            by = by % size
            if by == 0:
                return place[axis]
            target = place[axis] + by
            return jnp.where(target >= size, target - size, target)

        targets = {axis: [moved(axis, by) for by in range(sizes[axis])] for axis in AXES}

        def device(axes, offset):
            return {axis: targets[axis][by] for axis, by in zip(axes, offset)}

        barrier = pltpu.get_barrier_semaphore()
        count = 0
        for axes in stages[0]:
            for offset in offsets_of(axes, sizes):
                pl.semaphore_signal(
                    barrier, inc=1, device_id=device(axes, offset), device_id_type=MESH
                )
                count += 1
        load_euler = pltpu.make_async_copy(euler_hbm, euler_ref, load_sem.at[0])
        load_gravity = pltpu.make_async_copy(
            gravity_hbm, grav_bufs.at[0, pl.ds(0, 4)], load_sem.at[1]
        )
        load_euler.start()
        load_gravity.start()
        load_euler.wait()
        load_gravity.wait()

        plane = Plane(ny, nz)
        state = [[euler_ref[var, x] for x in range(nx)] for var in range(5)]
        grav = [[grav_bufs[0, var, x] for x in range(nx)] for var in range(4)]

        def pack(round_at, fields):
            lanes = [jnp.zeros((ny, nz), jnp.float32) for side in range(2)]
            for at, item in enumerate(itertools.chain(*fields)):
                send_y[round_at, 0, at : at + 1, :] = item[ny - 1 : ny, :]
                send_y[round_at, 1, at : at + 1, :] = item[0:1, :]
                here = plane.index[1] == at
                lanes[0] = jnp.where(here, plane.ahead(item, nz - 1 - at, 1), lanes[0])
                lanes[1] = jnp.where(here, plane.ahead(item, -at, 1), lanes[1])
            send_z[round_at, 0] = lanes[0]
            send_z[round_at, 1] = lanes[1]

        def exchange(round_at, vars_at):
            copies = []
            packed = (vars_at + 5 if round_at == 0 else vars_at) * nx
            rows = 8 * ((packed + 7) // 8)

            def send(src, dst, slot, axis, by):
                copy = pltpu.make_async_remote_copy(
                    src_ref=src,
                    dst_ref=dst,
                    send_sem=send_sem.at[round_at, slot],
                    recv_sem=recv_sem.at[round_at, slot],
                    device_id=device((axis,), (by % sizes[axis],)),
                    device_id_type=MESH,
                )
                copy.start()
                copies.append(copy)

            for side, by in ((0, 1), (1, -1)):
                face = nx - 1 if side == 0 else 0
                if round_at == 0:
                    send(euler_ref.at[:, face], halo_xe.at[side], 6 + side, "gx", by)
                send(
                    grav_bufs.at[round_at, pl.ds(0, vars_at), face],
                    halo_xg.at[round_at, side, pl.ds(0, vars_at)],
                    side,
                    "gx",
                    by,
                )
                send(
                    send_y.at[round_at, side, pl.ds(0, rows)],
                    recv_y.at[round_at, side, pl.ds(0, rows)],
                    2 + side,
                    "gy",
                    by,
                )
                send(send_z.at[round_at, side], recv_z.at[round_at, side], 4 + side, "gz", by)
            return copies

        def halo_y(round_at, side, at):
            return jnp.broadcast_to(recv_y[round_at, side, at : at + 1, :], (ny, nz))

        def halo_z(column, at):
            return jnp.broadcast_to(column[:, at : at + 1], (ny, nz))

        def reduce_start(round_at, stage_at, rows):
            axes = stages[round_at][stage_at]
            for at, row in enumerate(rows):
                reduce_send[round_at, stage_at, at] = row
            for slot, offset in enumerate(offsets_of(axes, sizes)):
                copy = pltpu.make_async_remote_copy(
                    src_ref=reduce_send.at[round_at, stage_at, pl.ds(0, len(rows))],
                    dst_ref=reduce_recv[round_at][stage_at].at[slot],
                    send_sem=reduce_send_sem.at[round_at, stage_at],
                    recv_sem=reduce_recv_sem.at[round_at, stage_at],
                    device_id=device(axes, offset),
                    device_id_type=MESH,
                )
                copy.start()

        def reduce_step(round_at, stage_at, rows, combine):
            got = reduce_recv[round_at][stage_at]
            pltpu.make_async_copy(got, got, reduce_recv_sem.at[round_at, stage_at]).wait()
            pltpu.make_async_copy(got, got, reduce_send_sem.at[round_at, stage_at]).wait()
            new_rows = []
            for at, row in enumerate(rows):
                parts = [row] + [got[slot, at] for slot in range(got.shape[0])]
                while len(parts) > 1:
                    pairs = [
                        combine[at](parts[item], parts[item + 1])
                        for item in range(0, len(parts) - 1, 2)
                    ]
                    parts = pairs + ([parts[-1]] if len(parts) % 2 else [])
                new_rows.append(parts[0])
            return new_rows

        pack(0, state + grav)
        nodes = [primitive([state[var][x] for var in range(5)]) for x in range(nx)]
        weight_yz = plane.coef(WEIGHTS, 0) * plane.coef(WEIGHTS, 1)

        def weighted_row(items):
            total = sum(float(WEIGHTS[x % 4]) * items[x] for x in range(nx))
            return jnp.sum(weight_yz * total, axis=0, keepdims=True)

        speeds = [
            jnp.abs(node[5]) + jnp.abs(node[6]) + jnp.abs(node[7]) + 3.0 * node[9] for node in nodes
        ]
        fastest = speeds[0]
        for item in speeds[1:]:
            fastest = jnp.maximum(fastest, item)
        first_rows = [jnp.max(fastest, axis=0, keepdims=True), weighted_row(state[0])]

        pl.semaphore_wait(barrier, count)
        copies_0 = exchange(0, 4)
        reduce_start(0, 0, first_rows)

        alpha = element_alpha(nodes, plane, nx)
        volume = [[None] * nx for var in range(5)]
        add_volume(volume, nodes, plane, nx)
        total = [[(1.0 - alpha[x]) * volume[var][x] for x in range(nx)] for var in range(5)]

        for copy in copies_0:
            copy.wait()
        first_combine = [jnp.maximum, jnp.add]
        first_rows = reduce_step(0, 0, first_rows, first_combine)
        reduce_start(0, 1, first_rows)

        def face_coefs(axis, alpha_x):
            start = jnp.where(plane.is_node[axis][0], 1.0, alpha_x)
            stop = jnp.where(plane.is_node[axis][3], 1.0, alpha_x)
            inverse = plane.coef(1.0 / WEIGHTS, axis)
            return start * inverse, stop * inverse

        edges = [primitive([halo_xe[side, var] for var in range(5)]) for side in range(2)]
        row = [edges[0]] + nodes + [edges[1]]
        faces = [euler_interface(row[at], row[at + 1], 0) for at in range(nx + 1)]
        for x in range(nx):
            node = x % 4
            start = 1.0 / WEIGHTS[0] if node == 0 else alpha[x] * float(1.0 / WEIGHTS[node])
            stop = 1.0 / WEIGHTS[3] if node == 3 else alpha[x] * float(1.0 / WEIGHTS[node])
            for var in range(5):
                total[var][x] += stop * faces[x + 1][var] - start * faces[x][var]
        column = [recv_z[0, side] for side in range(2)]
        for axis in range(2):
            for x in range(nx):
                start, stop = face_coefs(axis, alpha[x])
                halos = [
                    [
                        halo_y(0, side, var * nx + x)
                        if axis == 0
                        else halo_z(column[side], var * nx + x)
                        for var in range(5)
                    ]
                    for side in range(2)
                ]
                before = primitive(
                    [plane.previous(state[var][x], halos[0][var], axis) for var in range(5)]
                )
                after = primitive(
                    [plane.following(state[var][x], halos[1][var], axis) for var in range(5)]
                )
                left = euler_interface(before, nodes[x], axis + 1)
                right = euler_interface(nodes[x], after, axis + 1)
                for var in range(5):
                    total[var][x] += stop * right[var] - start * left[var]
        rate = [[-(2.0 / elem_width) * total[var][x] for x in range(nx)] for var in range(5)]
        for x in range(nx):
            for comp in range(3):
                rate[1 + comp][x] = rate[1 + comp][x] - state[0][x] * grav[1 + comp][x]
            rate[4][x] = rate[4][x] - (
                state[1][x] * grav[1][x] + state[2][x] * grav[2][x] + state[3][x] * grav[3][x]
            )
            for var in range(5):
                rate_ref[var, x] = rate[var][x]
        mass_row = weighted_row(rate[0])

        def gravity_rate(grav, drive):
            result = [[-coupling * drive[x] for x in range(nx)]]
            for comp in range(3):
                decay = grav[1 + comp]
                result.append(
                    [0.0] * nx
                    if decay[0] is None
                    else [-decay[x] / relax_time for x in range(nx)]
                )
            scale = -(2.0 / elem_width)
            for start in range(0, nx, 4):
                for node in range(4):
                    for other in range(4):
                        coef = float(-scale * DERIV_FOLDED[node, other])
                        if grav[1][0] is not None:
                            result[0][start + node] += coef * grav[1][start + other]
                        result[1][start + node] += coef / relax_time * grav[0][start + other]
            for axis in range(2):
                for x in range(nx):
                    matrix = -scale * DERIV_FOLDED
                    if grav[1][0] is not None:
                        result[0][x] += plane.apply(matrix, grav[2 + axis][x], axis)
                    result[2 + axis][x] += plane.apply(matrix / relax_time, grav[0][x], axis)
            return result, scale

        def gravity_faces(result, scale, grav, round_at, first_at, first_var):
            live = [var for var in range(4) if grav[var][0] is not None]

            def each(make):
                return [make(var) if var in live else None for var in range(4)]

            edges = [
                each(lambda var: halo_xg[round_at, side, first_var + var]) for side in range(2)
            ]
            row = [edges[0]] + [[grav[var][x] for var in range(4)] for x in range(nx)] + [edges[1]]
            for x in range(0, nx, 4):
                left = gravity_interface(row[x], row[x + 1], 0)
                right = gravity_interface(row[x + 4], row[x + 5], 0)
                for var in range(4):
                    if left[var] is not None:
                        result[var][x] += float(-scale / WEIGHTS[0]) * left[var]
                        result[var][x + 3] += float(scale / WEIGHTS[3]) * right[var]
            column = [recv_z[round_at, side] for side in range(2)]
            for axis in range(2):
                start = plane.coef([-scale / WEIGHTS[0], 0.0, 0.0, 0.0], axis)
                stop = plane.coef([0.0, 0.0, 0.0, scale / WEIGHTS[3]], axis)
                for x in range(nx):
                    halos = [
                        each(
                            lambda var: halo_y(round_at, side, first_at + var * nx + x)
                            if axis == 0
                            else halo_z(column[side], first_at + var * nx + x)
                        )
                        for side in range(2)
                    ]
                    here = [grav[var][x] for var in range(4)]
                    before = each(lambda var: plane.previous(here[var], halos[0][var], axis))
                    after = each(lambda var: plane.following(here[var], halos[1][var], axis))
                    left = gravity_interface(before, here, axis + 1)
                    right = gravity_interface(here, after, axis + 1)
                    for var in range(4):
                        if left[var] is not None:
                            result[var][x] += start * left[var] + stop * right[var]
            return result

        def step(old, change):
            return [
                [
                    pseudo_step * change[var][x]
                    if old[var][x] is None
                    else old[var][x] + pseudo_step * change[var][x]
                    for x in range(nx)
                ]
                for var in range(4)
            ]

        rate_grav, scale = gravity_rate(grav, state[0])
        rate_grav = gravity_faces(rate_grav, scale, grav, 0, 5 * nx, 0)
        none = [None] * nx
        more = [[(-pseudo_step * coupling) * rate[0][x] for x in range(nx)], none, none, none]
        for iteration in range(1, ITERS):
            grav = step(grav, rate_grav)
            if iteration > 1:
                more = step(more, rate_more)
            fields = grav + [items for items in more if items[0] is not None]
            for var, items in enumerate(fields):
                for x in range(nx):
                    grav_bufs[iteration, var, x] = items[x]
            pack(iteration, fields)
            copies = exchange(iteration, len(fields))
            rate_grav, scale = gravity_rate(grav, state[0])
            rate_more, scale = gravity_rate(more, rate[0])
            for copy in copies:
                copy.wait()
            if iteration < len(stages[0]):
                first_rows = reduce_step(0, iteration, first_rows, first_combine)
                if iteration + 1 < len(stages[0]):
                    reduce_start(0, iteration + 1, first_rows)
            rate_grav = gravity_faces(rate_grav, scale, grav, iteration, 0, 0)
            rate_more = gravity_faces(rate_more, scale, more, iteration, 4 * nx, 4)

        fastest = jnp.max(first_rows[0], axis=1, keepdims=True)
        mean_now = jnp.sum(first_rows[1], axis=1, keepdims=True) * (1.0 / weight_total)
        time_step = cfl_euler * elem_width / (7.0 * fastest)
        rate_phi = [
            rate_grav[0][x] + time_step * rate_more[0][x] + coupling * mean_now for x in range(nx)
        ]
        last_rows = [
            weighted_row([item * item for item in rate_phi]),
            weighted_row(rate_phi),
            mass_row,
        ]
        reduce_start(1, 0, last_rows)
        state_next = [
            [state[var][x] + time_step * rate[var][x] for x in range(nx)] for var in range(4)
        ]
        earlier = ((ITERS - 1) * pseudo_step * coupling) * mean_now
        phi = [
            grav[0][x] + time_step * more[0][x] + (pseudo_step * rate_phi[x] + earlier)
            for x in range(nx)
        ]
        grav, more = step(grav, rate_grav), step(more, rate_more)
        for x in range(nx):
            grad = [grav[1 + comp][x] + time_step * more[1 + comp][x] for comp in range(3)]
            for comp in range(3):
                grav_ref[1 + comp, x] = grad[comp]
                source_ref[comp, x] = -state_next[0][x] * grad[comp]
            source_ref[3, x] = -(
                state_next[1][x] * grad[0]
                + state_next[2][x] * grad[1]
                + state_next[3][x] * grad[2]
            )
        for stage_at in range(len(stages[1])):
            if stage_at > 0:
                reduce_start(1, stage_at, last_rows)
            last_rows = reduce_step(1, stage_at, last_rows, [jnp.add] * 3)
        squared, linear, mass = [jnp.sum(item, axis=1, keepdims=True) for item in last_rows]
        shift = coupling * (time_step * (mass * (1.0 / weight_total)))
        squared = squared + shift * (2.0 * linear + shift * weight_total)
        norm_ref[...] = jnp.sqrt(squared * (1.0 / weight_total))
        for x in range(nx):
            grav_ref[0, x] = phi[x] + (ITERS * pseudo_step) * shift

    rows_y = 8 * ((9 * nx + 7) // 8)
    plane_shape = (ny, nz)
    scratch = [
        pltpu.VMEM((5, nx) + plane_shape, jnp.float32),
        pltpu.VMEM((ITERS, 8, nx) + plane_shape, jnp.float32),
        pltpu.VMEM((2, 5) + plane_shape, jnp.float32),
        pltpu.VMEM((ITERS, 2, 8) + plane_shape, jnp.float32),
        pltpu.VMEM((ITERS, 2, rows_y, nz), jnp.float32),
        pltpu.VMEM((ITERS, 2, rows_y, nz), jnp.float32),
        pltpu.VMEM((ITERS, 2) + plane_shape, jnp.float32),
        pltpu.VMEM((ITERS, 2) + plane_shape, jnp.float32),
        pltpu.VMEM((2, len(stages[0]), 3, 1, nz), jnp.float32),
    ]
    for round_at, rows in enumerate((2, 3)):
        for axes in stages[round_at]:
            scratch.append(
                pltpu.VMEM((len(offsets_of(axes, sizes)), rows, 1, nz), jnp.float32)
            )
    scratch += [
        pltpu.SemaphoreType.DMA((2,)),
        pltpu.SemaphoreType.DMA((ITERS, 8)),
        pltpu.SemaphoreType.DMA((ITERS, 8)),
        pltpu.SemaphoreType.DMA((2, len(stages[0]))),
        pltpu.SemaphoreType.DMA((2, len(stages[0]))),
    ]
    return kernel, scratch


def solution(mesh):
    sizes = {axis: mesh.shape[axis] for axis in AXES}

    def local(euler_state, gravity_state):
        shape = euler_state.shape[1:]
        kernel, scratch = make_kernel(sizes, shape)
        vmem = pl.BlockSpec(memory_space=pltpu.VMEM)
        rate, gravity, source, norm = pl.pallas_call(
            kernel,
            out_shape=(
                pltpu.VMEM((5,) + shape, jnp.float32),
                pltpu.VMEM((4,) + shape, jnp.float32),
                pltpu.VMEM((4,) + shape, jnp.float32),
                jax.ShapeDtypeStruct((1, 1), jnp.float32),
            ),
            in_specs=[pl.BlockSpec(memory_space=pl.ANY)] * 2,
            out_specs=(vmem, vmem, vmem, vmem),
            scratch_shapes=scratch,
            compiler_params=pltpu.CompilerParams(collective_id=0, has_side_effects=True),
        )(euler_state, gravity_state)
        return rate, gravity, source, norm.reshape(())

    placed = (P(None, "gx", "gy", "gz"), P(None, "gx", "gy", "gz"))
    return jax.shard_map(
        local,
        mesh=mesh,
        in_specs=placed,
        out_specs=placed[:1] * 3 + (P(),),
        check_vma=False,
    )
```

```python
import itertools
import math

import jax
import jax.numpy as jnp
import numpy as np
from jax import lax
from jax.experimental import pallas as pl
from jax.experimental.pallas import tpu as pltpu
from jax.sharding import PartitionSpec as P

ITERS = 3
AXES = ("gx", "gy", "gz")
MOST_PARTNERS = 64

gamma_gas = 1.4
elem_width = 1.0
cfl_euler = 0.5
alpha_most = 0.5
indicator_level = 0.5 * 10.0 ** (-1.8 * 4.0**0.25)
indicator_slope = math.log((1.0 - 0.0001) / 0.0001) / indicator_level
coupling = 10.0
relax_time = 1.0
grav_speed = 1.0
pseudo_step = 0.3 * elem_width / 7.0
MESH = pl.DeviceIdType.MESH


def lgl_tables():
    points = np.array([-1.0, -1.0 / math.sqrt(5.0), 1.0 / math.sqrt(5.0), 1.0])
    weights = np.array([1.0, 5.0, 5.0, 1.0]) / 6.0
    barycentric = np.array(
        [
            1.0
            / np.prod([points[node_a] - points[node_b] for node_b in range(4) if node_b != node_a])
            for node_a in range(4)
        ]
    )
    derivative = np.zeros((4, 4))
    for node_a in range(4):
        for node_b in range(4):
            if node_b != node_a:
                derivative[node_a, node_b] = (
                    barycentric[node_b] / barycentric[node_a] / (points[node_a] - points[node_b])
                )
        derivative[node_a, node_a] = -np.sum(derivative[node_a])
    legendre = np.stack(
        [np.ones(4), points, 0.5 * (3.0 * points**2 - 1.0), 0.5 * (5.0 * points**3 - 3.0 * points)],
        axis=1,
    )
    legendre = legendre * np.sqrt((2.0 * np.arange(4) + 1.0) / 2.0)
    gram = np.sum(weights[:, None] * legendre * legendre, axis=0)
    modal_map = (legendre * weights[:, None]).T / gram[:, None]
    return (weights, derivative, modal_map)


WEIGHTS, DERIV, MODAL = lgl_tables()
DERIV_FOLDED = DERIV.copy()
DERIV_FOLDED[0, 0] += 1.0 / WEIGHTS[0]
DERIV_FOLDED[3, 3] -= 1.0 / WEIGHTS[3]
SELF_COEF = 2.0 * np.diag(DERIV)
SELF_COEF[0] += 1.0 / WEIGHTS[0]
SELF_COEF[3] -= 1.0 / WEIGHTS[3]


def reduce_stages(sizes):
    lines = [(axis,) for axis in AXES]
    total = math.prod(sizes[axis] for axis in AXES)
    return [lines, [AXES] if total <= MOST_PARTNERS else lines]


def offsets_of(axes, sizes):
    ranges = [range(sizes[axis]) for axis in axes]
    return [item for item in itertools.product(*ranges) if any(item)]


class Plane:
    def __init__(self, ny, nz):
        self.shape = (ny, nz)
        self.index = [lax.broadcasted_iota(jnp.int32, (ny, nz), axis) for axis in range(2)]
        self.node = [item & 3 for item in self.index]
        self.is_node = [[node == value for value in range(4)] for node in self.node]
        self.cache = {}

    def coef(self, values, axis):
        values = tuple(float(np.float32(value)) for value in values)
        if len(set(values)) == 1:
            return values[0]
        key = (values, axis)
        if key not in self.cache:
            result = jnp.full(self.shape, values[3], jnp.float32)
            for node in range(2, -1, -1):
                result = jnp.where(self.is_node[axis][node], values[node], result)
            self.cache[key] = result
        return self.cache[key]

    def ahead(self, value, by, axis):
        return pltpu.roll(value, (-by) % self.shape[axis], axis)

    def apply(self, matrix, value, axis):
        total = self.coef(np.diag(matrix), axis) * value
        for by in range(1, 4):
            up = [matrix[node, node + by] if node + by < 4 else 0.0 for node in range(4)]
            down = [matrix[node, node - by] if node - by >= 0 else 0.0 for node in range(4)]
            total = total + self.coef(up, axis) * self.ahead(value, by, axis)
            total = total + self.coef(down, axis) * self.ahead(value, -by, axis)
        return total

    def previous(self, value, halo, axis):
        return jnp.where(self.index[axis] == 0, halo, self.ahead(value, -1, axis))

    def following(self, value, halo, axis):
        last = self.shape[axis] - 1
        return jnp.where(self.index[axis] == last, halo, self.ahead(value, 1, axis))


def primitive(state):
    inverse = 1.0 / state[0]
    vel = [state[1 + comp] * inverse for comp in range(3)]
    kinetic = state[1] * vel[0] + state[2] * vel[1] + state[3] * vel[2]
    pressure = (gamma_gas - 1.0) * (state[4] - 0.5 * kinetic)
    sound = jnp.sqrt(gamma_gas * pressure * inverse)
    return list(state) + vel + [pressure, sound]


def flux_of(node, direction):
    normal = node[5 + direction]
    momentum = [
        node[1 + comp] * normal + node[8] if comp == direction else node[1 + comp] * normal
        for comp in range(3)
    ]
    return [node[1 + direction]] + momentum + [(node[4] + node[8]) * normal]


def euler_interface(left, right, direction):
    speed = 0.5 * jnp.maximum(
        jnp.abs(left[5 + direction]) + left[9], jnp.abs(right[5 + direction]) + right[9]
    )
    flux_left, flux_right = flux_of(left, direction), flux_of(right, direction)
    return [
        0.5 * (flux_left[var] + flux_right[var]) - speed * (right[var] - left[var])
        for var in range(5)
    ]


def log_mean_parts(left, right):
    total = left + right
    ratio = (left - right) / total
    ratio_sq = ratio * ratio
    is_close = ratio_sq < 0.0001
    series = 2.0 + ratio_sq * (2.0 / 3.0 + ratio_sq * (2.0 / 5.0 + ratio_sq * (2.0 / 7.0)))
    top = jnp.where(is_close, total, right - left)
    low = jnp.where(is_close, series, jnp.log(right / left))
    return top, low


def two_point(left, right, direction):
    top, low = log_mean_parts(left[0], right[0])
    rho_mean = top / low
    top, low = log_mean_parts(left[0] * right[4], right[0] * left[4])
    inv_mean = left[4] * right[4] * low / top
    vel_avg = [0.5 * (left[1 + comp] + right[1 + comp]) for comp in range(3)]
    pres_avg = 0.5 * (left[4] + right[4])
    vel_product = 0.5 * (left[1] * right[1] + left[2] * right[2] + left[3] * right[3])
    mass = rho_mean * vel_avg[direction]
    momentum = [
        mass * vel_avg[comp] + pres_avg if comp == direction else mass * vel_avg[comp]
        for comp in range(3)
    ]
    energy = mass * (vel_product + inv_mean * (1.0 / (gamma_gas - 1.0))) + 0.5 * (
        left[4] * right[1 + direction] + right[4] * left[1 + direction]
    )
    return [mass] + momentum + [energy]


def gravity_interface(left, right, direction):
    result = []
    for var in range(4):
        parts = []
        other = 1 + direction if var == 0 else 0
        if var in (0, 1 + direction) and left[other] is not None:
            parts.append(-(0.5 / relax_time if var else 0.5) * (left[other] + right[other]))
        if left[var] is not None:
            parts.append((-0.5 * grav_speed) * (right[var] - left[var]))
        result.append(sum(parts[1:], parts[0]) if parts else None)
    return result


def add_volume(volume, nodes, plane, nx):
    pair_fields = [[node[0], node[5], node[6], node[7], node[8]] for node in nodes]

    def add(x, terms):
        for var in range(5):
            old = volume[var][x]
            volume[var][x] = terms[var] if old is None else old + terms[var]

    for start in range(0, nx, 4):
        for low in range(4):
            own = flux_of(nodes[start + low], 0)
            coef = float(np.float32(SELF_COEF[low]))
            add(start + low, [coef * item for item in own])
            for high in range(low + 1, 4):
                flux = two_point(pair_fields[start + low], pair_fields[start + high], 0)
                add(start + low, [float(2.0 * DERIV[low, high]) * item for item in flux])
                add(start + high, [float(2.0 * DERIV[high, low]) * item for item in flux])
    deriv = 2.0 * DERIV
    for axis in range(2):
        direction = axis + 1
        for x in range(nx):
            here = pair_fields[x]
            own = flux_of(nodes[x], direction)
            coef = plane.coef(SELF_COEF, axis)
            add(x, [coef * item for item in own])
            there = [plane.ahead(item, 1, axis) for item in here]
            flux = two_point(here, there, direction)
            up = plane.coef([deriv[0, 1], deriv[1, 2], deriv[2, 3], 0.0], axis)
            down = plane.coef([0.0, deriv[1, 0], deriv[2, 1], deriv[3, 2]], axis)
            add(x, [up * item + down * plane.ahead(item, -1, axis) for item in flux])
            is_last = plane.is_node[axis][3]
            there = [
                jnp.where(is_last, plane.ahead(item, -3, axis), plane.ahead(item, 2, axis))
                for item in here
            ]
            flux = two_point(here, there, direction)
            own_coef = plane.coef([deriv[0, 2], deriv[1, 3], 0.0, deriv[3, 0]], axis)
            down = plane.coef([0.0, 0.0, deriv[2, 0], deriv[3, 1]], axis)
            up = plane.coef([deriv[0, 3], 0.0, 0.0, 0.0], axis)
            add(
                x,
                [
                    own_coef * item
                    + down * plane.ahead(item, -2, axis)
                    + up * plane.ahead(item, 3, axis)
                    for item in flux
                ],
            )


def element_alpha(nodes, plane, nx):
    ones = np.ones((4, 4))
    low_index = np.array([1.0, 1.0, 1.0, 0.0])
    not_low = 1.0 - plane.coef(low_index, 0) * plane.coef(low_index, 1)
    result = []
    for start in range(0, nx, 4):
        product = [nodes[start + node][0] * nodes[start + node][8] for node in range(4)]
        energies = []
        for mode in range(4):
            coeffs = sum(float(MODAL[mode, node]) * product[node] for node in range(4))
            coeffs = plane.apply(MODAL, plane.apply(MODAL, coeffs, 0), 1)
            energies.append(coeffs * coeffs)
        low_part = energies[0] + energies[1] + energies[2]
        sums = [low_part + energies[3], low_part * not_low + energies[3]]
        sums = [plane.apply(ones, plane.apply(ones, item, 1), 0) for item in sums]
        share = sums[1] / sums[0]
        alpha = alpha_most / (1.0 + jnp.exp(-indicator_slope * (share - indicator_level)))
        result += [alpha] * 4
    return result


def make_kernel(sizes, shape):
    nx, ny, nz = shape
    stages = reduce_stages(sizes)
    weight_total = (
        8.0 * (nx // 4) * (ny // 4) * (nz // 4) * math.prod(sizes[axis] for axis in AXES)
    )

    def kernel(
        euler_hbm,
        gravity_hbm,
        rate_ref,
        grav_ref,
        source_ref,
        norm_ref,
        euler_ref,
        grav_bufs,
        halo_xe,
        halo_xg,
        send_y,
        recv_y,
        send_z,
        recv_z,
        reduce_send,
        *rest,
    ):
        reduce_recv = [rest[: len(stages[0])], rest[len(stages[0]) : -5]]
        load_sem, send_sem, recv_sem, reduce_send_sem, reduce_recv_sem = rest[-5:]
        place = {axis: lax.axis_index(axis) for axis in AXES}

        def moved(axis, by):
            size = sizes[axis]
            by = by % size
            if by == 0:
                return place[axis]
            target = place[axis] + by
            return jnp.where(target >= size, target - size, target)

        targets = {axis: [moved(axis, by) for by in range(sizes[axis])] for axis in AXES}

        def device(axes, offset):
            return {axis: targets[axis][by] for axis, by in zip(axes, offset)}

        barrier = pltpu.get_barrier_semaphore()
        count = 0
        for axes in stages[0]:
            for offset in offsets_of(axes, sizes):
                pl.semaphore_signal(
                    barrier, inc=1, device_id=device(axes, offset), device_id_type=MESH
                )
                count += 1
        load_euler = pltpu.make_async_copy(euler_hbm, euler_ref, load_sem.at[0])
        load_gravity = pltpu.make_async_copy(
            gravity_hbm, grav_bufs.at[0, pl.ds(0, 4)], load_sem.at[1]
        )
        load_euler.start()
        load_gravity.start()
        load_euler.wait()
        load_gravity.wait()

        plane = Plane(ny, nz)
        state = [[euler_ref[var, x] for x in range(nx)] for var in range(5)]
        grav = [[grav_bufs[0, var, x] for x in range(nx)] for var in range(4)]

        def pack(round_at, fields):
            lanes = [jnp.zeros((ny, nz), jnp.float32) for side in range(2)]
            for at, item in enumerate(itertools.chain(*fields)):
                send_y[round_at, 0, at : at + 1, :] = item[ny - 1 : ny, :]
                send_y[round_at, 1, at : at + 1, :] = item[0:1, :]
                here = plane.index[1] == at
                lanes[0] = jnp.where(here, plane.ahead(item, nz - 1 - at, 1), lanes[0])
                lanes[1] = jnp.where(here, plane.ahead(item, -at, 1), lanes[1])
            send_z[round_at, 0] = lanes[0]
            send_z[round_at, 1] = lanes[1]

        def exchange(round_at, vars_at):
            copies = []
            packed = (vars_at + 5 if round_at == 0 else vars_at) * nx
            rows = 8 * ((packed + 7) // 8)

            def send(src, dst, slot, axis, by):
                copy = pltpu.make_async_remote_copy(
                    src_ref=src,
                    dst_ref=dst,
                    send_sem=send_sem.at[round_at, slot],
                    recv_sem=recv_sem.at[round_at, slot],
                    device_id=device((axis,), (by % sizes[axis],)),
                    device_id_type=MESH,
                )
                copy.start()
                copies.append(copy)

            for side, by in ((0, 1), (1, -1)):
                face = nx - 1 if side == 0 else 0
                if round_at == 0:
                    send(euler_ref.at[:, face], halo_xe.at[side], 6 + side, "gx", by)
                send(
                    grav_bufs.at[round_at, pl.ds(0, vars_at), face],
                    halo_xg.at[round_at, side, pl.ds(0, vars_at)],
                    side,
                    "gx",
                    by,
                )
                send(
                    send_y.at[round_at, side, pl.ds(0, rows)],
                    recv_y.at[round_at, side, pl.ds(0, rows)],
                    2 + side,
                    "gy",
                    by,
                )
                send(send_z.at[round_at, side], recv_z.at[round_at, side], 4 + side, "gz", by)
            return copies

        def halo_y(round_at, side, at):
            return jnp.broadcast_to(recv_y[round_at, side, at : at + 1, :], (ny, nz))

        def halo_z(column, at):
            return jnp.broadcast_to(column[:, at : at + 1], (ny, nz))

        def reduce_start(round_at, stage_at, rows):
            axes = stages[round_at][stage_at]
            for at, row in enumerate(rows):
                reduce_send[round_at, stage_at, at] = row
            for slot, offset in enumerate(offsets_of(axes, sizes)):
                copy = pltpu.make_async_remote_copy(
                    src_ref=reduce_send.at[round_at, stage_at, pl.ds(0, len(rows))],
                    dst_ref=reduce_recv[round_at][stage_at].at[slot],
                    send_sem=reduce_send_sem.at[round_at, stage_at],
                    recv_sem=reduce_recv_sem.at[round_at, stage_at],
                    device_id=device(axes, offset),
                    device_id_type=MESH,
                )
                copy.start()

        def reduce_step(round_at, stage_at, rows, combine):
            got = reduce_recv[round_at][stage_at]
            pltpu.make_async_copy(got, got, reduce_recv_sem.at[round_at, stage_at]).wait()
            pltpu.make_async_copy(got, got, reduce_send_sem.at[round_at, stage_at]).wait()
            new_rows = []
            for at, row in enumerate(rows):
                parts = [row] + [got[slot, at] for slot in range(got.shape[0])]
                while len(parts) > 1:
                    pairs = [
                        combine[at](parts[item], parts[item + 1])
                        for item in range(0, len(parts) - 1, 2)
                    ]
                    parts = pairs + ([parts[-1]] if len(parts) % 2 else [])
                new_rows.append(parts[0])
            return new_rows

        pack(0, state + grav)
        nodes = [primitive([state[var][x] for var in range(5)]) for x in range(nx)]
        weight_yz = plane.coef(WEIGHTS, 0) * plane.coef(WEIGHTS, 1)

        def weighted_row(items):
            total = sum(float(WEIGHTS[x % 4]) * items[x] for x in range(nx))
            return jnp.sum(weight_yz * total, axis=0, keepdims=True)

        speeds = [
            jnp.abs(node[5]) + jnp.abs(node[6]) + jnp.abs(node[7]) + 3.0 * node[9] for node in nodes
        ]
        fastest = speeds[0]
        for item in speeds[1:]:
            fastest = jnp.maximum(fastest, item)
        first_rows = [jnp.max(fastest, axis=0, keepdims=True), weighted_row(state[0])]

        pl.semaphore_wait(barrier, count)
        copies_0 = exchange(0, 4)
        reduce_start(0, 0, first_rows)

        alpha = element_alpha(nodes, plane, nx)
        volume = [[None] * nx for var in range(5)]
        add_volume(volume, nodes, plane, nx)
        total = [[(1.0 - alpha[x]) * volume[var][x] for x in range(nx)] for var in range(5)]

        for copy in copies_0:
            copy.wait()
        first_combine = [jnp.maximum, jnp.add]
        first_rows = reduce_step(0, 0, first_rows, first_combine)
        reduce_start(0, 1, first_rows)

        def face_coefs(axis, alpha_x):
            start = jnp.where(plane.is_node[axis][0], 1.0, alpha_x)
            stop = jnp.where(plane.is_node[axis][3], 1.0, alpha_x)
            inverse = plane.coef(1.0 / WEIGHTS, axis)
            return start * inverse, stop * inverse

        edges = [primitive([halo_xe[side, var] for var in range(5)]) for side in range(2)]
        row = [edges[0]] + nodes + [edges[1]]
        faces = [euler_interface(row[at], row[at + 1], 0) for at in range(nx + 1)]
        for x in range(nx):
            node = x % 4
            start = 1.0 / WEIGHTS[0] if node == 0 else alpha[x] * float(1.0 / WEIGHTS[node])
            stop = 1.0 / WEIGHTS[3] if node == 3 else alpha[x] * float(1.0 / WEIGHTS[node])
            for var in range(5):
                total[var][x] += stop * faces[x + 1][var] - start * faces[x][var]
        column = [recv_z[0, side] for side in range(2)]
        for axis in range(2):
            for x in range(nx):
                start, stop = face_coefs(axis, alpha[x])
                halos = [
                    [
                        halo_y(0, side, var * nx + x)
                        if axis == 0
                        else halo_z(column[side], var * nx + x)
                        for var in range(5)
                    ]
                    for side in range(2)
                ]
                before = primitive(
                    [plane.previous(state[var][x], halos[0][var], axis) for var in range(5)]
                )
                after = primitive(
                    [plane.following(state[var][x], halos[1][var], axis) for var in range(5)]
                )
                left = euler_interface(before, nodes[x], axis + 1)
                right = euler_interface(nodes[x], after, axis + 1)
                for var in range(5):
                    total[var][x] += stop * right[var] - start * left[var]
        rate = [[-(2.0 / elem_width) * total[var][x] for x in range(nx)] for var in range(5)]
        for x in range(nx):
            for comp in range(3):
                rate[1 + comp][x] = rate[1 + comp][x] - state[0][x] * grav[1 + comp][x]
            rate[4][x] = rate[4][x] - (
                state[1][x] * grav[1][x] + state[2][x] * grav[2][x] + state[3][x] * grav[3][x]
            )
            for var in range(5):
                rate_ref[var, x] = rate[var][x]
        mass_row = weighted_row(rate[0])

        def gravity_rate(grav, drive):
            result = [[-coupling * drive[x] for x in range(nx)]]
            for comp in range(3):
                decay = grav[1 + comp]
                result.append(
                    [0.0] * nx
                    if decay[0] is None
                    else [-decay[x] / relax_time for x in range(nx)]
                )
            scale = -(2.0 / elem_width)
            for start in range(0, nx, 4):
                for node in range(4):
                    for other in range(4):
                        coef = float(-scale * DERIV_FOLDED[node, other])
                        if grav[1][0] is not None:
                            result[0][start + node] += coef * grav[1][start + other]
                        result[1][start + node] += coef / relax_time * grav[0][start + other]
            for axis in range(2):
                for x in range(nx):
                    matrix = -scale * DERIV_FOLDED
                    if grav[1][0] is not None:
                        result[0][x] += plane.apply(matrix, grav[2 + axis][x], axis)
                    result[2 + axis][x] += plane.apply(matrix / relax_time, grav[0][x], axis)
            return result, scale

        def gravity_faces(result, scale, grav, round_at, first_at, first_var):
            live = [var for var in range(4) if grav[var][0] is not None]

            def each(make):
                return [make(var) if var in live else None for var in range(4)]

            edges = [
                each(lambda var: halo_xg[round_at, side, first_var + var]) for side in range(2)
            ]
            row = [edges[0]] + [[grav[var][x] for var in range(4)] for x in range(nx)] + [edges[1]]
            for x in range(0, nx, 4):
                left = gravity_interface(row[x], row[x + 1], 0)
                right = gravity_interface(row[x + 4], row[x + 5], 0)
                for var in range(4):
                    if left[var] is not None:
                        result[var][x] += float(-scale / WEIGHTS[0]) * left[var]
                        result[var][x + 3] += float(scale / WEIGHTS[3]) * right[var]
            column = [recv_z[round_at, side] for side in range(2)]
            for axis in range(2):
                start = plane.coef([-scale / WEIGHTS[0], 0.0, 0.0, 0.0], axis)
                stop = plane.coef([0.0, 0.0, 0.0, scale / WEIGHTS[3]], axis)
                for x in range(nx):
                    halos = [
                        each(
                            lambda var: halo_y(round_at, side, first_at + var * nx + x)
                            if axis == 0
                            else halo_z(column[side], first_at + var * nx + x)
                        )
                        for side in range(2)
                    ]
                    here = [grav[var][x] for var in range(4)]
                    before = each(lambda var: plane.previous(here[var], halos[0][var], axis))
                    after = each(lambda var: plane.following(here[var], halos[1][var], axis))
                    left = gravity_interface(before, here, axis + 1)
                    right = gravity_interface(here, after, axis + 1)
                    for var in range(4):
                        if left[var] is not None:
                            result[var][x] += start * left[var] + stop * right[var]
            return result

        def step(old, change):
            return [
                [
                    pseudo_step * change[var][x]
                    if old[var][x] is None
                    else old[var][x] + pseudo_step * change[var][x]
                    for x in range(nx)
                ]
                for var in range(4)
            ]

        rate_grav, scale = gravity_rate(grav, state[0])
        rate_grav = gravity_faces(rate_grav, scale, grav, 0, 5 * nx, 0)
        none = [None] * nx
        more = [[(-pseudo_step * coupling) * rate[0][x] for x in range(nx)], none, none, none]
        for iteration in range(1, ITERS):
            grav = step(grav, rate_grav)
            if iteration > 1:
                more = step(more, rate_more)
            fields = grav + [items for items in more if items[0] is not None]
            for var, items in enumerate(fields):
                for x in range(nx):
                    grav_bufs[iteration, var, x] = items[x]
            pack(iteration, fields)
            copies = exchange(iteration, len(fields))
            rate_grav, scale = gravity_rate(grav, state[0])
            rate_more, scale = gravity_rate(more, rate[0])
            for copy in copies:
                copy.wait()
            if iteration < len(stages[0]):
                first_rows = reduce_step(0, iteration, first_rows, first_combine)
                if iteration + 1 < len(stages[0]):
                    reduce_start(0, iteration + 1, first_rows)
            rate_grav = gravity_faces(rate_grav, scale, grav, iteration, 0, 0)
            rate_more = gravity_faces(rate_more, scale, more, iteration, 4 * nx, 4)

        fastest = jnp.max(first_rows[0], axis=1, keepdims=True)
        mean_now = jnp.sum(first_rows[1], axis=1, keepdims=True) * (1.0 / weight_total)
        time_step = cfl_euler * elem_width / (7.0 * fastest)
        rate_phi = [
            rate_grav[0][x] + time_step * rate_more[0][x] + coupling * mean_now for x in range(nx)
        ]
        last_rows = [
            weighted_row([item * item for item in rate_phi]),
            weighted_row(rate_phi),
            mass_row,
        ]
        reduce_start(1, 0, last_rows)
        state_next = [
            [state[var][x] + time_step * rate[var][x] for x in range(nx)] for var in range(4)
        ]
        earlier = ((ITERS - 1) * pseudo_step * coupling) * mean_now
        phi = [
            grav[0][x] + time_step * more[0][x] + (pseudo_step * rate_phi[x] + earlier)
            for x in range(nx)
        ]
        grav, more = step(grav, rate_grav), step(more, rate_more)
        for x in range(nx):
            grad = [grav[1 + comp][x] + time_step * more[1 + comp][x] for comp in range(3)]
            for comp in range(3):
                grav_ref[1 + comp, x] = grad[comp]
                source_ref[comp, x] = -state_next[0][x] * grad[comp]
            source_ref[3, x] = -(
                state_next[1][x] * grad[0]
                + state_next[2][x] * grad[1]
                + state_next[3][x] * grad[2]
            )
        for stage_at in range(len(stages[1])):
            if stage_at > 0:
                reduce_start(1, stage_at, last_rows)
            last_rows = reduce_step(1, stage_at, last_rows, [jnp.add] * 3)
        squared, linear, mass = [jnp.sum(item, axis=1, keepdims=True) for item in last_rows]
        shift = coupling * (time_step * (mass * (1.0 / weight_total)))
        squared = squared + shift * (2.0 * linear + shift * weight_total)
        norm_ref[...] = jnp.sqrt(squared * (1.0 / weight_total))
        for x in range(nx):
            grav_ref[0, x] = phi[x] + (ITERS * pseudo_step) * shift

    rows_y = 8 * ((9 * nx + 7) // 8)
    plane_shape = (ny, nz)
    scratch = [
        pltpu.VMEM((5, nx) + plane_shape, jnp.float32),
        pltpu.VMEM((ITERS, 8, nx) + plane_shape, jnp.float32),
        pltpu.VMEM((2, 5) + plane_shape, jnp.float32),
        pltpu.VMEM((ITERS, 2, 8) + plane_shape, jnp.float32),
        pltpu.VMEM((ITERS, 2, rows_y, nz), jnp.float32),
        pltpu.VMEM((ITERS, 2, rows_y, nz), jnp.float32),
        pltpu.VMEM((ITERS, 2) + plane_shape, jnp.float32),
        pltpu.VMEM((ITERS, 2) + plane_shape, jnp.float32),
        pltpu.VMEM((2, len(stages[0]), 3, 1, nz), jnp.float32),
    ]
    for round_at, rows in enumerate((2, 3)):
        for axes in stages[round_at]:
            scratch.append(
                pltpu.VMEM((len(offsets_of(axes, sizes)), rows, 1, nz), jnp.float32)
            )
    scratch += [
        pltpu.SemaphoreType.DMA((2,)),
        pltpu.SemaphoreType.DMA((ITERS, 8)),
        pltpu.SemaphoreType.DMA((ITERS, 8)),
        pltpu.SemaphoreType.DMA((2, len(stages[0]))),
        pltpu.SemaphoreType.DMA((2, len(stages[0]))),
    ]
    return kernel, scratch


def solution(mesh):
    sizes = {axis: mesh.shape[axis] for axis in AXES}

    def local(euler_state, gravity_state):
        shape = euler_state.shape[1:]
        kernel, scratch = make_kernel(sizes, shape)
        vmem = pl.BlockSpec(memory_space=pltpu.VMEM)
        rate, gravity, source, norm = pl.pallas_call(
            kernel,
            out_shape=(
                pltpu.VMEM((5,) + shape, jnp.float32),
                pltpu.VMEM((4,) + shape, jnp.float32),
                pltpu.VMEM((4,) + shape, jnp.float32),
                pltpu.VMEM((1, 1), jnp.float32),
            ),
            in_specs=[pl.BlockSpec(memory_space=pl.ANY)] * 2,
            out_specs=(vmem, vmem, vmem, vmem),
            scratch_shapes=scratch,
            compiler_params=pltpu.CompilerParams(collective_id=0, has_side_effects=True),
        )(euler_state, gravity_state)
        return rate, gravity, source, norm.reshape(())

    placed = (P(None, "gx", "gy", "gz"), P(None, "gx", "gy", "gz"))
    return jax.shard_map(
        local,
        mesh=mesh,
        in_specs=placed,
        out_specs=placed[:1] * 3 + (P(),),
        check_vma=False,
    )
```
